32 devices in a mesh: rep: 2 (over y), seq: 16 (over z, x, core).
Axes of the slice: x: 2, y: 2, z: 4, core: 2. Of those that a mesh axis runs over, the one named last changes fastest.
Arguments:
- latents: bfloat16 [16, 24576], P(None, ('rep', 'seq')), parts along dimension 1, may hold values from -6 to 6
- layout: int32 [32, 768], P('rep'), parts along dimension 0, may hold values from 0 to 12287, as said below
- assign: int32 [16], P('rep'), parts along dimension 0, may hold values from 0 to 7, as said below
- counts: int32 [16], P('rep'), parts along dimension 0, may hold values from 1 to 3
- latent_cache: bfloat16 [2, 128, 1024], P(None, ('rep', 'seq')), parts along dimension 1, may hold values from -6 to 6
- feature_cache: bfloat16 [2, 128, 64, 384], P(None, ('rep', 'seq')), parts along dimension 1, may hold values from -4 to 4
- first_weight: bfloat16 [3, 3, 3, 16, 384], replicated, may hold values from -0.3125 to 0.3125
- first_bias: float32 [384], replicated, may hold values from -3 to 3
- norm_gain: float32 [384], replicated, may hold values from 0.25 to 1.75
- second_weight: bfloat16 [3, 3, 3, 384, 192], replicated, may hold values from -0.0625 to 0.0625
- second_bias: float32 [192], replicated, may hold values from -3 to 3
Outputs:
- decoded_frames: bfloat16 [3, 256, 128, 192], P(None, ('rep', 'seq')), parts along dimension 1
- latent_cache_next: bfloat16 [2, 128, 1024], P(None, ('rep', 'seq')), parts along dimension 1
- feature_cache_next: bfloat16 [2, 128, 64, 384], P(None, ('rep', 'seq')), parts along dimension 1
The draws below stay inside these ranges and needn't reach their ends.
There are 2 independent parts, one for each index of `rep`. The reference program is written for one: setup_inputs(seed, part) draws one part's arguments, and reference() takes and returns one part's arrays. A program takes and returns all parts, laid end to end along the dimension named above; an argument that names none is the same for every part. Nothing has to cross between parts.
Inputs may be any that keep to these rules, and one draw needn't show every extreme that they name: assign is a permutation of 0 to 7. layout is a permutation of 0 to 12287. Call the cells of request assign[g], rows k * 4 to (k + 1) * 4 - 1, all frames and columns, the tile of seq index (g * 2 + k - 1) mod 16; every row of layout holds exactly 48 cells of every tile.
All inputs are finite; a program needn't handle non-finite values.
Results may differ from the reference program's by a relative error of at most 0.0034.
Values may be sent and summed in bfloat16 or wider, within the bound.
A program may use at most 128 MiB of HBM per device.

```python
import jax
import jax.numpy as jnp
from jax import lax

LAT_CH = 16
MID_CH = 384
OUT_CH = 192
REQS = 8
FMAX = 3
ROWS_DEV = 4
W = 64
GROUP = 2
SHIFT = 1
HEIGHT = 8
CELLS = 768
PEER = 48
TOTAL_CELLS = 12288
ROWS_ALL = 64
N_SEQ = 16


def pairing(key):
    return jax.random.permutation(jax.random.fold_in(key, 11), REQS).astype(jnp.int32)


def one_permutation(subkey):
    return jax.random.permutation(subkey, CELLS).astype(jnp.int32)


def draw_assign(key, part):
    return pairing(key)


def draw_layout(key, part):
    assign = pairing(key)
    spread_keys = jax.random.split(jax.random.fold_in(key, 23), N_SEQ)
    within = jax.vmap(one_permutation)(spread_keys)
    numbers = jnp.arange(N_SEQ, dtype=jnp.int32)[:, None] * CELLS + within
    numbers = jnp.transpose(numbers.reshape(N_SEQ, N_SEQ, PEER), (1, 0, 2)).reshape(N_SEQ, CELLS)
    slot_keys = jax.random.split(jax.random.fold_in(key, 37), N_SEQ)
    mixing = jax.vmap(one_permutation)(slot_keys)
    numbers = jnp.take_along_axis(numbers, mixing, axis=1)
    target = numbers // CELLS
    inside = numbers % CELLS
    frame_index = inside // (ROWS_DEV * W)
    tile_row = inside // W % ROWS_DEV
    column = inside % W
    place = (target + SHIFT) % N_SEQ
    group_index = place // GROUP
    position = place % GROUP
    request = jnp.take(assign, group_index)
    image_row = position * ROWS_DEV + tile_row
    return (((request * FMAX + frame_index) * HEIGHT + image_row) * W + column).astype(jnp.int32)


def plant(entries, key, smallest, top_value):
    spot = [jax.random.randint(jax.random.fold_in(key, axis), (), 0, length) for axis, length in enumerate(entries.shape)]
    longest = entries.shape.index(max(entries.shape))
    neighbour = spot[:longest] + [(spot[longest] + 1) % entries.shape[longest]] + spot[longest + 1:]
    return entries.at[tuple(spot)].set(smallest).at[tuple(neighbour)].set(top_value)


def levels(rng, extent, cuts, low, largest):
    factor_of = 1.0
    for axis_at, blocks in cuts:
        draws = jax.random.uniform(jax.random.fold_in(jax.random.fold_in(rng, 6), axis_at), (blocks,), jnp.float32, low / len(cuts), largest / len(cuts))
        factor_of = factor_of * jnp.repeat(jnp.exp(draws), extent[axis_at] // blocks).reshape((-1,) + (1,) * (len(extent) - 1 - axis_at))
    return factor_of


def scatter_about(key, shape, deviation, bound, pieces=(), kind=jnp.bfloat16):
    values = jax.random.normal(key, shape, jnp.float32) * deviation
    if len(pieces) > 0:
        values = levels(key, shape, pieces, -0.22, 0.18) * values
    return jnp.clip(values, min=-bound, max=bound).astype(kind)


def setup_inputs(seed: int = 0, part: int = 0) -> dict:
    key_of = jax.random.split(jax.random.key(seed), 12)
    part_keys = jax.random.split(jax.random.fold_in(key_of[11], part), 12)
    return {
        "latents": scatter_about(part_keys[0], (LAT_CH, TOTAL_CELLS), 1.0, 6.0, ((1, 16),)),
        "layout": draw_layout(jax.random.fold_in(jax.random.fold_in(key_of[11], part), 71), part),
        "assign": draw_assign(jax.random.fold_in(jax.random.fold_in(key_of[11], part), 71), part),
        "counts": plant(jax.random.randint(part_keys[3], (REQS,), 1, FMAX + 1), jax.random.fold_in(part_keys[3], 1), 1, FMAX).astype(jnp.int32),
        "latent_cache": scatter_about(part_keys[4], (2, ROWS_ALL, W * LAT_CH), 1.0, 6.0, ((1, 16),)),
        "feature_cache": scatter_about(part_keys[5], (2, ROWS_ALL, W, MID_CH), 0.6, 4.0, ((1, 16),)),
        "first_weight": scatter_about(key_of[6], (3, 3, 3, LAT_CH, MID_CH), (27 * LAT_CH) ** -0.5, 0.3125),
        "first_bias": scatter_about(key_of[7], (MID_CH,), 0.5, 3.0, (), jnp.float32),
        "norm_gain": jnp.clip(1.0 + 0.15 * jax.random.normal(key_of[8], (MID_CH,), jnp.float32), 0.25, 1.75),
        "second_weight": scatter_about(key_of[9], (3, 3, 3, MID_CH, OUT_CH), (27 * MID_CH) ** -0.5, 0.0625),
        "second_bias": scatter_about(key_of[10], (OUT_CH,), 0.5, 3.0, (), jnp.float32),
    }


def causal_conv(values, weight, offset):
    result = lax.conv_general_dilated(values[None], weight, (1, 1, 1), ((0, 0), (1, 1), (1, 1)), dimension_numbers=('NDHWC', 'DHWIO', 'NDHWC'), preferred_element_type=jnp.float32)
    return result[0] + offset

def activate(linear, norm_gain):
    inverse = lax.rsqrt(lax.optimization_barrier(jnp.mean(linear * linear, axis=-1, keepdims=True)) + 1e-06)
    return jax.nn.silu(linear * inverse * norm_gain).astype(jnp.bfloat16)

def reference(latents, layout, assign, counts, latent_cache, feature_cache, first_weight, first_bias, norm_gain, second_weight, second_bias):
    positions = jnp.argsort(layout.reshape(-1)).astype(jnp.int32)
    ordered = jnp.take(latents, positions, axis=1).reshape(LAT_CH, REQS, FMAX, HEIGHT, W)
    ordered = jnp.transpose(ordered, (1, 2, 3, 4, 0))
    latent_prev = jnp.roll(latent_cache, SHIFT * ROWS_DEV, axis=1).reshape(2, REQS, HEIGHT, W, LAT_CH)
    feature_prev = jnp.roll(feature_cache, SHIFT * ROWS_DEV, axis=1).reshape(2, REQS, HEIGHT, W, MID_CH)
    frame_index = jnp.arange(FMAX, dtype=jnp.int32)[:, None, None, None]
    decoded_list = []
    latent_list = []
    feature_list = []
    for group_index in range(REQS):
        request = assign[group_index].astype(jnp.int32)
        live_frames = counts[request].astype(jnp.int32)
        window = lax.dynamic_index_in_dim(ordered, request, 0, keepdims=False)
        first_input = jnp.concatenate([latent_prev[:, group_index], window], axis=0)
        features = activate(causal_conv(first_input, first_weight, first_bias), norm_gain)
        second_input = jnp.concatenate([feature_prev[:, group_index], features], axis=0)
        doubled = jnp.repeat(jnp.repeat(second_input, 2, axis=1), 2, axis=2)
        decoded = causal_conv(doubled, second_weight, second_bias)
        decoded = jnp.where(frame_index < live_frames, decoded, 0.0).astype(jnp.bfloat16)
        decoded_list.append(decoded)
        latent_list.append(lax.dynamic_slice_in_dim(first_input, live_frames, 2, 0))
        feature_list.append(lax.dynamic_slice_in_dim(second_input, live_frames, 2, 0))
    decoded_frames = jnp.roll(jnp.concatenate(decoded_list, axis=1), -2 * SHIFT * ROWS_DEV, axis=1)
    latent_cache_next = jnp.roll(jnp.concatenate(latent_list, axis=1), -SHIFT * ROWS_DEV, axis=1).reshape(2, ROWS_ALL, W * LAT_CH)
    feature_cache_next = jnp.roll(jnp.concatenate(feature_list, axis=1), -SHIFT * ROWS_DEV, axis=1)
    return (decoded_frames, latent_cache_next, feature_cache_next)
```

```python
import functools

import jax
import jax.numpy as jnp
from jax import lax
from jax.experimental import pallas as pl
from jax.experimental.pallas import tpu as pltpu
from jax.sharding import PartitionSpec as P

LAT_CH = 16
REQS = 8
FMAX = 3
ROWS_DEV = 4
W = 64
F32 = jnp.float32
BF16 = jnp.bfloat16


def lane_index(shape):
    return lax.broadcasted_iota(jnp.int32, shape, len(shape) - 1)


def column_of(row, lanes):
    return jnp.transpose(jnp.broadcast_to(row, (lanes, row.shape[1])))


def sublane_index(shape):
    return lax.broadcasted_iota(jnp.int32, shape, len(shape) - 2)


def trips(count, step, carry=None):
    body = lambda i, c: step(i) or 0
    lax.fori_loop(0, count, body, 0, unroll=True if count <= 16 else 1)


def ranks_in(mask, before):
    rows, slots = mask.shape
    blocks = slots // 128
    stacked = jnp.concatenate([mask[:, i * 128 : i * 128 + 128] for i in range(blocks)], axis=0)
    counted = jnp.dot(stacked.astype(BF16), before, preferred_element_type=F32)
    base = jnp.zeros((rows, 128), F32)
    ranks = []
    for i in range(blocks):
        block = counted[i * rows : (i + 1) * rows]
        ranks.append(block[:, 0:128] + base)
        base = base + block[:, 128:256]
    return jnp.where(mask > 0.0, jnp.concatenate(ranks, axis=1), -1.0)


def place_of(device, devices, per_group):
    place = lax.rem(device + per_group // 2, devices)
    return place // per_group, lax.rem(place, per_group)


def exchange_kernel(
    devices,
    assign,
    latents,
    layout,
    latent_cache,
    feature_cache,
    first,
    halo,
    outgoing,
    incoming,
    past,
    edges,
    row_line,
    row_column,
    row_rank,
    line_mask,
    column_hot,
    send_sem,
    recv_sem,
    edge_send,
    edge_recv,
    halo_send,
    halo_recv,
):
    me = lax.axis_index("seq")
    per_group = devices // REQS
    slots = layout.shape[1]
    history, inner, wide = latent_cache.shape
    height = inner * per_group
    span = min(3, per_group)
    starts = per_group - span + 1
    used = -(-span * (slots // devices) // 16) * 16
    lines = FMAX * (inner + 4)
    group, position = place_of(me, devices, per_group)
    above = lax.rem(me + devices - 1, devices)
    below = lax.rem(me + 1, devices)

    barrier = pltpu.get_barrier_semaphore()

    def greet(i):
        pl.semaphore_signal(barrier, inc=1, device_id={"seq": lax.rem(me + 1 + i, devices)})

    trips(devices - 1, greet)

    for f in range(history):
        stacked = []
        for r in range(inner):
            row = jnp.broadcast_to(latent_cache[f, r : r + 1, :].astype(F32), (LAT_CH, wide))
            mine = sublane_index(row.shape) == lane_index(row.shape) % LAT_CH
            stacked.append(jnp.where(mine, row, 0.0).astype(BF16))
        pick = sublane_index((wide, 128)) // LAT_CH == lane_index((wide, 128)) % W
        turned = jnp.dot(
            jnp.concatenate(stacked, axis=0), pick.astype(BF16), preferred_element_type=F32
        ).astype(BF16)
        for r in range(0, inner, 2):
            low = turned[r * LAT_CH : (r + 1) * LAT_CH]
            high = turned[(r + 1) * LAT_CH : (r + 2) * LAT_CH]
            left = lane_index(low.shape) < W
            past[f, r // 2] = jnp.where(left, low, high)

    square = (128, 256)
    earlier = (sublane_index(square) < lane_index(square)) | (lane_index(square) >= 128)
    before = earlier.astype(BF16)
    mine = layout[pl.ds(me, 1), :]
    remain = mine // W
    row = lax.rem(remain, height)
    step = remain // height
    windows = REQS * starts
    window = sublane_index((windows, slots))
    request = jnp.zeros((windows, slots), jnp.int32)
    for g in range(REQS):
        request = jnp.where(window // starts == g, assign[g], request)
    low = lax.rem(window, starts) * inner
    member = (step >= request * FMAX) & (step < request * FMAX + FMAX)
    member = member & (row >= low) & (row < low + span * inner)
    rank = ranks_in(jnp.where(member, 1.0, 0.0), before)
    row_rank[0:windows] = rank

    def chosen(i):
        ranked = row_rank[pl.ds(i, 1), :]
        hot = sublane_index((used, slots)).astype(F32) == ranked
        hot = jnp.where(hot, 1.0, 0.0).astype(BF16)
        if used < 128:
            hot = jnp.concatenate([hot, jnp.zeros((128 - used, slots), BF16)], axis=0)
        return hot

    def collect(i):
        hot = jnp.concatenate([chosen(2 * i), chosen(2 * i + 1)], axis=0)
        moved = lax.dot_general(
            latents[...], hot, (((1,), (1,)), ((), ())), preferred_element_type=F32
        ).astype(BF16)
        outgoing[2 * i] = moved[:, 0:128]
        outgoing[2 * i + 1] = moved[:, 128:256]

    trips(windows // 2, collect)

    pl.semaphore_wait(barrier, devices - 1)

    def window_of(device):
        g, k = place_of(device, devices, per_group)
        return g * starts + jnp.clip(k - 1, 0, starts - 1)

    def copy_to(i):
        peer = lax.rem(me + 1 + i, devices)
        return pltpu.make_async_remote_copy(
            src_ref=outgoing.at[window_of(peer)],
            dst_ref=incoming.at[me],
            send_sem=send_sem.at[peer],
            recv_sem=recv_sem.at[me],
            device_id={"seq": peer},
        )

    trips(devices - 1, lambda i: copy_to(i).start())

    def edge_copies(side):
        peer = (above, below)[side]
        copies = []
        for f in range(history):
            copies.append(
                pltpu.make_async_remote_copy(
                    src_ref=past.at[f, 0 if side == 0 else inner // 2 - 1],
                    dst_ref=edges.at[1 - side, f],
                    send_sem=edge_send.at[side, f],
                    recv_sem=edge_recv.at[1 - side, f],
                    device_id={"seq": peer},
                )
            )
            copies.append(
                pltpu.make_async_remote_copy(
                    src_ref=feature_cache.at[f, 0 if side == 0 else inner - 1],
                    dst_ref=halo.at[1 - side, f],
                    send_sem=halo_send.at[side, f],
                    recv_sem=halo_recv.at[1 - side, f],
                    device_id={"seq": peer},
                )
            )
        return copies

    has = (position > 0, position < per_group - 1)
    for side in range(2):

        @pl.when(has[side])
        def _start():
            for copy in edge_copies(side):
                copy.start()

    incoming[me] = outgoing[window_of(me)]

    number = layout[...]
    remain = number // W
    row = lax.rem(remain, height)
    step = remain // height - assign[group] * FMAX
    first_tile = jnp.clip(position - 1, 0, starts - 1)
    member = (step >= 0) & (step < FMAX)
    member = member & (row >= first_tile * inner) & (row < (first_tile + span) * inner)
    rank = ranks_in(jnp.where(member, 1.0, 0.0), before)
    local = row - (position * inner - 2)
    line = jnp.where((local >= 0) & (local < inner + 4), step * (inner + 4) + local + 1, 0)
    row_rank[0:devices] = rank
    row_line[...] = line.astype(F32)
    row_column[...] = lax.rem(number, W).astype(F32)

    def locate(i):
        ranked = row_rank[pl.ds(i, 1), :]
        hot = sublane_index((128, slots)).astype(F32) == ranked
        hot = jnp.where(hot, 1.0, 0.0).astype(BF16)
        shape = (16, slots)
        what = jnp.where(
            sublane_index(shape) == 0, row_line[pl.ds(i, 1), :], row_column[pl.ds(i, 1), :]
        ).astype(BF16)
        found = lax.dot_general(what, hot, (((1,), (1,)), ((), ())), preferred_element_type=F32)
        level = sublane_index((lines * LAT_CH, 128)) // LAT_CH + 1
        line_mask[i] = jnp.where(level.astype(F32) == found[0:1], 1.0, 0.0).astype(BF16)
        column = jnp.transpose(jnp.broadcast_to(found[1:2], (128, 128)))
        same = column == (lane_index((128, 128)) % W).astype(F32)
        column_hot[pl.ds(pl.multiple_of(i * 128, 128), 128)] = jnp.where(same, 1.0, 0.0).astype(BF16)

    trips(devices, locate)

    for side in range(2):

        @pl.when(jnp.logical_not(has[side]))
        def _clear():
            edges[side] = jnp.zeros(edges.shape[1:], BF16)

        @pl.when(has[side])
        def _arrive():
            for copy in edge_copies(1 - side):
                copy.wait_recv()

    def arrive(i):
        peer = lax.rem(me + 1 + i, devices)
        pltpu.make_async_remote_copy(
            src_ref=outgoing.at[0],
            dst_ref=incoming.at[peer],
            send_sem=send_sem.at[peer],
            recv_sem=recv_sem.at[peer],
            device_id={"seq": peer},
        ).wait_recv()

    trips(devices - 1, arrive)

    def place(i, total):
        pieces = []
        for half in range(2):
            got = incoming[2 * i + half]
            pieces.append(jnp.concatenate([got] * lines, axis=0) * line_mask[2 * i + half])
        hot = column_hot[pl.ds(pl.multiple_of(i * 256, 256), 256)]
        return total + jnp.dot(jnp.concatenate(pieces, axis=1), hot, preferred_element_type=F32)

    pairs = devices // 2
    placed = lax.fori_loop(
        0,
        pairs,
        place,
        jnp.zeros((lines * LAT_CH, 128), F32),
        unroll=True if pairs <= 16 else 1,
    )
    left = lane_index((LAT_CH, 128)) < W
    block = (inner + 4) * W
    for i in range(lines // 2):
        low = placed[2 * i * LAT_CH : (2 * i + 1) * LAT_CH]
        high = placed[(2 * i + 1) * LAT_CH : (2 * i + 2) * LAT_CH]
        start = history * block + i * 128
        first[:, start : start + 128] = jnp.where(left, low, high).astype(BF16)
    for f in range(history):
        first[:, f * block : f * block + 128] = edges[0, f]
        for r in range(inner // 2):
            start = f * block + 128 + r * 128
            first[:, start : start + 128] = past[f, r]
        first[:, f * block + block - 128 : f * block + block] = edges[1, f]

    trips(devices - 1, lambda i: copy_to(i).wait_send())
    for side in range(2):

        @pl.when(has[side])
        def _sent():
            for copy in edge_copies(side):
                copy.wait_send()


def exchange(assign, latents, layout, latent_cache, feature_cache):
    devices, slots = layout.shape
    history, inner, _, mid = feature_cache.shape
    per_group = devices // REQS
    windows = REQS * (per_group - min(3, per_group) + 1)
    lines = FMAX * (inner + 4)
    vmem = pl.BlockSpec(memory_space=pltpu.VMEM)
    return pl.pallas_call(
        functools.partial(exchange_kernel, devices),
        in_specs=[pl.BlockSpec(memory_space=pltpu.SMEM), vmem, vmem, vmem, pl.BlockSpec(memory_space=pl.ANY)],
        out_specs=[vmem, pl.BlockSpec(memory_space=pl.ANY)],
        out_shape=[
            jax.ShapeDtypeStruct((LAT_CH, (history + FMAX) * (inner + 4) * W), BF16),
            jax.ShapeDtypeStruct((2, history, W, mid), BF16),
        ],
        scratch_shapes=[
            pltpu.VMEM((windows, LAT_CH, 128), BF16),
            pltpu.VMEM((devices, LAT_CH, 128), BF16),
            pltpu.VMEM((history, inner // 2, LAT_CH, 128), BF16),
            pltpu.VMEM((2, history, LAT_CH, 128), BF16),
            pltpu.VMEM((devices, slots), F32),
            pltpu.VMEM((devices, slots), F32),
            pltpu.VMEM((max(devices, windows), slots), F32),
            pltpu.VMEM((devices, lines * LAT_CH, 128), BF16),
            pltpu.VMEM((devices * 128, 128), BF16),
            pltpu.SemaphoreType.DMA((devices,)),
            pltpu.SemaphoreType.DMA((devices,)),
            pltpu.SemaphoreType.DMA((2, history)),
            pltpu.SemaphoreType.DMA((2, history)),
            pltpu.SemaphoreType.DMA((2, history)),
            pltpu.SemaphoreType.DMA((2, history)),
        ],
        compiler_params=pltpu.CompilerParams(
            collective_id=0, has_side_effects=True, vmem_limit_bytes=48 * 1024 * 1024
        ),
    )(assign, latents, layout, latent_cache, feature_cache)


def decode_kernel(
    assign, counts, first, cached, halo, w1, b1, gain, w2, b2, out, carry, latent_next, feat, packed, pre, columns
):
    frame = pl.program_id(0)
    history, inner, _, mid = cached.shape
    width = b2.shape[0]
    rows = inner + 2
    cells = inner * W
    devices = lax.axis_size("seq")
    per_group = devices // REQS
    group, position = place_of(lax.axis_index("seq"), devices, per_group)
    has = (position > 0, position < per_group - 1)
    count = counts[assign[group]]
    span = rows * W
    frames = FMAX

    col = lane_index((16, span)) % W
    keep = ((col != 0).astype(BF16), None, (col != W - 1).astype(BF16))

    def spread(f, value, ch, count):
        value = value.astype(BF16)
        for e in range(3):
            whole = value if e == 1 else pltpu.roll(value, (1, 0, span - 1)[e], 1) * keep[e]
            feat[e, f, pl.ds(ch, count), 0:span] = whole
            below = pltpu.roll(value, span - W + 1 - e, 1)[:, 0:cells]
            feat[e, f, pl.ds(ch, count), span : span + cells] = below if e == 1 else below * keep[e][:, 0:cells]

    @pl.when(frame == 0)
    def _prepare():
        def pack(step, _):
            at = pl.multiple_of(step * 16, 16)
            for a in range(3):
                taps = [
                    [w2[a, b, e, pl.ds(at, 16), :].astype(F32) for e in range(3)] for b in range(3)
                ]
                for py in range(2):
                    if py == 0:
                        lines = (taps[0], [taps[1][e] + taps[2][e] for e in range(3)])
                    else:
                        lines = ([taps[0][e] + taps[1][e] for e in range(3)], taps[2])
                    for px in range(2):
                        for iy, line in enumerate(lines):
                            if px == 0:
                                pair = (line[0], line[1] + line[2])
                            else:
                                pair = (line[0] + line[1], line[2])
                            for ix, value in enumerate(pair):
                                start = ((a * 2 + iy) * 2 + ix) * mid
                                packed[2 * py + px, pl.ds(at, 16), start : start + mid] = value.astype(BF16)
            return 0

        lax.fori_loop(0, width // 16, pack, 0)

        columns[0, 0:mid] = column_of(b1[...].reshape(1, mid), 128)
        columns[1, 0:mid] = column_of(gain[...].reshape(1, mid), 128)
        columns[2, 0:width] = column_of(b2[...].reshape(1, width), 128)

        for f in range(history):
            sides = [jnp.where(has[i], halo[i, f], jnp.zeros((), BF16)) for i in range(2)]
            tall = jnp.concatenate([sides[0], cached[f].reshape(cells, mid), sides[1]], axis=0)
            pre[...] = jnp.transpose(tall.astype(F32))

            def turn(step, _):
                at = pl.multiple_of(step * 16, 16)
                spread(f, pre[pl.ds(at, 16), :], at, 16)
                return 0

            lax.fori_loop(0, mid // 16, turn, 0, unroll=True)

        value = first[...].astype(F32)
        total = value.shape[1]
        col = lane_index(value.shape) % W
        left = jnp.where(col == 0, 0.0, pltpu.roll(value, 1, 1))
        right = jnp.where(col == W - 1, 0.0, pltpu.roll(value, total - 1, 1))
        shifts = [v.astype(BF16) for v in (left, value, right)]
        later = [pltpu.roll(v, total - W, 1).astype(BF16) for v in (left, value, right)]
        block = (rows + 2) * W
        row = lane_index((16, span)) // W
        outside = ((row == 0) & jnp.logical_not(has[0])) | ((row == rows - 1) & jnp.logical_not(has[1]))
        for t in range(frames):
            patch = []
            for a in range(3):
                for b in range(3):
                    source, begin = (later, 0) if b == 1 else (shifts, b * W)
                    begin += (t + a) * block
                    for e in range(3):
                        patch.append(source[e][:, begin : begin + span])
            pre[...] = lax.dot_general(
                w1[...].reshape(27 * LAT_CH, mid),
                jnp.concatenate(patch, axis=0),
                (((0,), (0,)), ((), ())),
                preferred_element_type=F32,
            )

            def square(step, acc):
                at = pl.multiple_of(step * 16, 16)
                bias = columns[0, pl.ds(at, 16)]
                x = pre[pl.ds(at, 16), :] + jnp.concatenate([bias] * (span // 128), axis=1)
                pre[pl.ds(at, 16), :] = x
                return acc + x * x

            squares = lax.fori_loop(0, mid // 16, square, jnp.zeros((16, span), F32), unroll=True)
            inverse = lax.rsqrt(jnp.sum(squares, axis=0, keepdims=True) / mid + 1e-06)

            def finish(step, _):
                at = pl.multiple_of(step * 16, 16)
                scale = columns[1, pl.ds(at, 16)]
                x = pre[pl.ds(at, 16), :] * inverse * jnp.concatenate([scale] * (span // 128), axis=1)
                x = x / (1.0 + jnp.exp(-x))
                spread(history + t, jnp.where(outside, 0.0, x), at, 16)
                return 0

            lax.fori_loop(0, mid // 16, finish, 0, unroll=True)

        live = count
        for i in range(history):
            carry[i] = jnp.transpose(feat[1, live + i, :, span : span + cells].astype(F32)).astype(
                BF16
            ).reshape(inner, W, mid)
        parts = []
        for i in range(history):
            start = pl.multiple_of((live + i) * block + 2 * W, 128)
            own = first[:, pl.ds(start, cells)].astype(F32)
            for r in range(inner):
                parts.append(own[:, r * W : (r + 1) * W])
        stacked = jnp.concatenate(parts, axis=0).astype(BF16)
        pick = lax.broadcasted_iota(jnp.int32, (W, W * LAT_CH), 0) == lane_index((W, W * LAT_CH)) // LAT_CH
        wide = jnp.dot(stacked, pick.astype(BF16), preferred_element_type=F32)
        wide = wide.reshape(history * inner, LAT_CH, W * LAT_CH)
        mine = lax.broadcasted_iota(jnp.int32, wide.shape, 1) == lane_index(wide.shape) % LAT_CH
        latent_next[...] = (
            jnp.sum(jnp.where(mine, wide, 0.0), axis=1).astype(BF16).reshape(history, inner, W * LAT_CH)
        )

    live = frame < count
    pair = 2 * W
    spot = lax.broadcasted_iota(jnp.int32, (2 * pair, 2 * pair), 0)
    goal = spot // pair + 2 * (spot % pair)
    mix = (lane_index((2 * pair, 2 * pair)) == goal).astype(BF16)
    bias = jnp.concatenate([columns[2, 0:width]] * (cells // 128), axis=1)
    for py in range(2):
        halves = []
        for px in range(2):
            parts = []
            for a in range(3):
                for iy in range(2):
                    begin = (0, span, 2 * W)[py + iy]
                    for ix in range(2):
                        parts.append(feat[px + ix, frame + a, :, begin : begin + cells])
            total = jnp.dot(
                packed[2 * py + px], jnp.concatenate(parts, axis=0), preferred_element_type=F32
            )
            halves.append(jnp.where(live, total + bias, 0.0).astype(BF16))
        for i in range(0, inner, 2):
            both = jnp.concatenate([half[:, i * W : i * W + pair] for half in halves], axis=1)
            mixed = jnp.dot(both, mix, preferred_element_type=F32).astype(BF16)
            out[0, 2 * i + py] = mixed[:, 0:pair]
            out[0, 2 * i + 2 + py] = mixed[:, pair : 2 * pair]


def decode(assign, counts, first, cached, halo, w1, b1, gain, w2, b2):
    history, inner, _, mid = cached.shape
    width = b2.shape[0]
    rows = inner + 2
    frames = FMAX
    whole = lambda array: pl.BlockSpec(array.shape, lambda t: (0,) * array.ndim)
    return pl.pallas_call(
        decode_kernel,
        grid=(frames,),
        in_specs=[pl.BlockSpec(memory_space=pltpu.SMEM)] * 2
        + [whole(array) for array in (first, cached, halo, w1, b1, gain, w2, b2)],
        out_specs=[
            pl.BlockSpec((1, 2 * inner, width, 2 * W), lambda t: (t, 0, 0, 0)),
            pl.BlockSpec((history, inner, W, mid), lambda t: (0, 0, 0, 0)),
            pl.BlockSpec((history, inner, W * LAT_CH), lambda t: (0, 0, 0)),
        ],
        out_shape=[
            jax.ShapeDtypeStruct((frames, 2 * inner, width, 2 * W), BF16),
            jax.ShapeDtypeStruct((history, inner, W, mid), BF16),
            jax.ShapeDtypeStruct((history, inner, W * LAT_CH), BF16),
        ],
        scratch_shapes=[
            pltpu.VMEM((3, history + frames, mid, (rows + inner) * W), BF16),
            pltpu.VMEM((4, width, 12 * mid), BF16),
            pltpu.VMEM((mid, rows * W), F32),
            pltpu.VMEM((3, mid, 128), F32),
        ],
        compiler_params=pltpu.CompilerParams(
            dimension_semantics=("arbitrary",), vmem_limit_bytes=56 * 1024 * 1024
        ),
        cost_estimate=pl.CostEstimate(
            flops=2 * frames * inner * W * 48 * mid * width,
            bytes_accessed=8_000_000,
            transcendentals=0,
        ),
    )(assign, counts, first, cached, halo, w1, b1, gain, w2, b2)


def body(
    latents,
    layout,
    assign,
    counts,
    latent_cache,
    feature_cache,
    first_weight,
    first_bias,
    norm_gain,
    second_weight,
    second_bias,
):
    first, halo = exchange(assign, latents, layout, latent_cache, feature_cache)
    decoded_frames, feature_next, latent_next = decode(
        assign,
        counts,
        first,
        feature_cache,
        halo,
        first_weight,
        first_bias,
        norm_gain,
        jnp.swapaxes(second_weight, 3, 4),
        second_bias,
    )
    return (jnp.swapaxes(decoded_frames, 2, 3), latent_next, feature_next)


def solution(mesh):
    return jax.shard_map(
        body,
        mesh=mesh,
        in_specs=(
            P(None, ("rep", "seq")),
            P("rep", None),
            P("rep"),
            P("rep"),
            P(None, ("rep", "seq"), None),
            P(None, ("rep", "seq"), None, None),
            P(),
            P(),
            P(),
            P(),
            P(),
        ),
        out_specs=(
            P(None, ("rep", "seq"), None, None),
            P(None, ("rep", "seq"), None),
            P(None, ("rep", "seq"), None, None),
        ),
        check_vma=False,
    )
```

```python
import functools

import jax
import jax.numpy as jnp
from jax import lax
from jax.experimental import pallas as pl
from jax.experimental.pallas import tpu as pltpu
from jax.sharding import PartitionSpec as P

LAT_CH = 16
REQS = 8
FMAX = 3
ROWS_DEV = 4
W = 64
F32 = jnp.float32
BF16 = jnp.bfloat16


def lane_index(shape):
    return lax.broadcasted_iota(jnp.int32, shape, len(shape) - 1)


def in_hbm(array):
    return pltpu.with_memory_space_constraint(array, pltpu.HBM)


def column_of(row, lanes):
    return jnp.transpose(jnp.broadcast_to(row, (lanes, row.shape[1])))


def sublane_index(shape):
    return lax.broadcasted_iota(jnp.int32, shape, len(shape) - 2)


def trips(count, step, carry=None):
    body = lambda i, c: step(i) or 0
    lax.fori_loop(0, count, body, 0, unroll=True if count <= 16 else 1)


def ranks_in(mask, before):
    rows, slots = mask.shape
    blocks = slots // 128
    stacked = jnp.concatenate([mask[:, i * 128 : i * 128 + 128] for i in range(blocks)], axis=0)
    counted = jnp.dot(stacked.astype(BF16), before, preferred_element_type=F32)
    base = jnp.zeros((rows, 128), F32)
    ranks = []
    for i in range(blocks):
        block = counted[i * rows : (i + 1) * rows]
        ranks.append(block[:, 0:128] + base)
        base = base + block[:, 128:256]
    return jnp.where(mask > 0.0, jnp.concatenate(ranks, axis=1), -1.0)


def place_of(device, devices, per_group):
    place = lax.rem(device + per_group // 2, devices)
    return place // per_group, lax.rem(place, per_group)


def section_kernel(
    devices,
    assign_hbm,
    latents_hbm,
    layout_hbm,
    latent_cache_hbm,
    feature_cache_hbm,
    w1_hbm,
    b1_hbm,
    gain_hbm,
    w2_hbm,
    b2_hbm,
    halves,
    center,
    first,
    assign,
    latents,
    layout,
    latent_cache,
    feature_cache,
    w1,
    b1,
    gain,
    w2,
    b2,
    halo,
    outgoing,
    incoming,
    past,
    edges,
    row_line,
    row_column,
    row_rank,
    line_mask,
    column_hot,
    feat,
    packed,
    partial,
    pre,
    columns,
    load_sem,
    send_sem,
    recv_sem,
    edge_send,
    edge_recv,
    halo_send,
    halo_recv,
):
    me = lax.axis_index("seq")
    per_group = devices // REQS
    slots = layout.shape[1]
    history, inner, wide = latent_cache.shape
    height = inner * per_group
    span = min(3, per_group)
    starts = per_group - span + 1
    used = -(-span * (slots // devices) // 16) * 16
    lines = FMAX * (inner + 4)
    group, position = place_of(me, devices, per_group)
    above = lax.rem(me + devices - 1, devices)
    below = lax.rem(me + 1, devices)

    loads = [
        pltpu.make_async_copy(source, target, load_sem.at[i])
        for i, (source, target) in enumerate(
            (
                (assign_hbm, assign),
                (layout_hbm, layout),
                (latents_hbm, latents),
                (latent_cache_hbm, latent_cache),
                (feature_cache_hbm, feature_cache),
                (w2_hbm, w2),
                (w1_hbm, w1),
                (b1_hbm, b1),
                (gain_hbm, gain),
                (b2_hbm, b2),
            )
        )
    ]
    for load in loads:
        load.start()

    barrier = pltpu.get_barrier_semaphore()

    def greet(i):
        pl.semaphore_signal(barrier, inc=1, device_id={"seq": lax.rem(me + 1 + i, devices)})

    trips(devices - 1, greet)

    for load in loads[0:4]:
        load.wait()

    for f in range(history):
        stacked = []
        for r in range(inner):
            row = jnp.broadcast_to(latent_cache[f, r : r + 1, :].astype(F32), (LAT_CH, wide))
            mine = sublane_index(row.shape) == lane_index(row.shape) % LAT_CH
            stacked.append(jnp.where(mine, row, 0.0).astype(BF16))
        pick = sublane_index((wide, 128)) // LAT_CH == lane_index((wide, 128)) % W
        turned = jnp.dot(
            jnp.concatenate(stacked, axis=0), pick.astype(BF16), preferred_element_type=F32
        ).astype(BF16)
        for r in range(0, inner, 2):
            low = turned[r * LAT_CH : (r + 1) * LAT_CH]
            high = turned[(r + 1) * LAT_CH : (r + 2) * LAT_CH]
            left = lane_index(low.shape) < W
            past[f, r // 2] = jnp.where(left, low, high)

    square = (128, 256)
    earlier = (sublane_index(square) < lane_index(square)) | (lane_index(square) >= 128)
    before = earlier.astype(BF16)
    mine = layout[pl.ds(me, 1), :]
    remain = mine // W
    row = lax.rem(remain, height)
    step = remain // height
    windows = REQS * starts
    window = sublane_index((windows, slots))
    request = jnp.zeros((windows, slots), jnp.int32)
    for g in range(REQS):
        request = jnp.where(window // starts == g, assign[g], request)
    low = lax.rem(window, starts) * inner
    member = (step >= request * FMAX) & (step < request * FMAX + FMAX)
    member = member & (row >= low) & (row < low + span * inner)
    rank = ranks_in(jnp.where(member, 1.0, 0.0), before)
    row_rank[0:windows] = rank

    def chosen(i):
        ranked = row_rank[pl.ds(i, 1), :]
        hot = sublane_index((used, slots)).astype(F32) == ranked
        hot = jnp.where(hot, 1.0, 0.0).astype(BF16)
        if used < 128:
            hot = jnp.concatenate([hot, jnp.zeros((128 - used, slots), BF16)], axis=0)
        return hot

    def collect(i):
        hot = jnp.concatenate([chosen(2 * i), chosen(2 * i + 1)], axis=0)
        moved = lax.dot_general(
            latents[...], hot, (((1,), (1,)), ((), ())), preferred_element_type=F32
        ).astype(BF16)
        outgoing[2 * i] = moved[:, 0:128]
        outgoing[2 * i + 1] = moved[:, 128:256]

    trips(windows // 2, collect)

    pl.semaphore_wait(barrier, devices - 1)

    def window_of(device):
        g, k = place_of(device, devices, per_group)
        return g * starts + jnp.clip(k - 1, 0, starts - 1)

    def copy_to(i):
        peer = lax.rem(me + 1 + i, devices)
        return pltpu.make_async_remote_copy(
            src_ref=outgoing.at[window_of(peer)],
            dst_ref=incoming.at[me],
            send_sem=send_sem.at[peer],
            recv_sem=recv_sem.at[me],
            device_id={"seq": peer},
        )

    trips(devices - 1, lambda i: copy_to(i).start())
    for load in loads[4:]:
        load.wait()

    def edge_copies(side):
        peer = (above, below)[side]
        copies = []
        for f in range(history):
            copies.append(
                pltpu.make_async_remote_copy(
                    src_ref=past.at[f, 0 if side == 0 else inner // 2 - 1],
                    dst_ref=edges.at[1 - side, f],
                    send_sem=edge_send.at[side, f],
                    recv_sem=edge_recv.at[1 - side, f],
                    device_id={"seq": peer},
                )
            )
            copies.append(
                pltpu.make_async_remote_copy(
                    src_ref=feature_cache.at[f, 0 if side == 0 else inner - 1],
                    dst_ref=halo.at[1 - side, f],
                    send_sem=halo_send.at[side, f],
                    recv_sem=halo_recv.at[1 - side, f],
                    device_id={"seq": peer},
                )
            )
        return copies

    has = (position > 0, position < per_group - 1)
    for side in range(2):

        @pl.when(has[side])
        def _start():
            for copy in edge_copies(side):
                copy.start()

    incoming[me] = outgoing[window_of(me)]

    number = layout[...]
    remain = number // W
    row = lax.rem(remain, height)
    step = remain // height - assign[group] * FMAX
    first_tile = jnp.clip(position - 1, 0, starts - 1)
    member = (step >= 0) & (step < FMAX)
    member = member & (row >= first_tile * inner) & (row < (first_tile + span) * inner)
    rank = ranks_in(jnp.where(member, 1.0, 0.0), before)
    local = row - (position * inner - 2)
    line = jnp.where((local >= 0) & (local < inner + 4), step * (inner + 4) + local + 1, 0)
    row_rank[0:devices] = rank
    row_line[...] = line.astype(F32)
    row_column[...] = lax.rem(number, W).astype(F32)

    def locate(i):
        ranked = row_rank[pl.ds(i, 1), :]
        hot = sublane_index((128, slots)).astype(F32) == ranked
        hot = jnp.where(hot, 1.0, 0.0).astype(BF16)
        shape = (16, slots)
        what = jnp.where(
            sublane_index(shape) == 0, row_line[pl.ds(i, 1), :], row_column[pl.ds(i, 1), :]
        ).astype(BF16)
        found = lax.dot_general(what, hot, (((1,), (1,)), ((), ())), preferred_element_type=F32)
        level = sublane_index((lines * LAT_CH, 128)) // LAT_CH + 1
        line_mask[i] = jnp.where(level.astype(F32) == found[0:1], 1.0, 0.0).astype(BF16)
        column = jnp.transpose(jnp.broadcast_to(found[1:2], (128, 128)))
        same = column == (lane_index((128, 128)) % W).astype(F32)
        column_hot[pl.ds(pl.multiple_of(i * 128, 128), 128)] = jnp.where(same, 1.0, 0.0).astype(BF16)

    trips(devices, locate)

    mid = feature_cache.shape[3]
    width = b2.shape[0]
    cells = inner * W
    high_rows = inner + 2
    stretch = high_rows * W
    col = lane_index((16, stretch)) % W
    keep = ((col != 0).astype(BF16), None, (col != W - 1).astype(BF16))

    shifted = (feat.at[0], center, feat.at[1])

    def spread(f, value, ch):
        value = value.astype(BF16)
        for e in range(3):
            whole = value if e == 1 else pltpu.roll(value, (1, 0, stretch - 1)[e], 1) * keep[e]
            shifted[e][f, ch : ch + 16, 0:stretch] = whole
            below = pltpu.roll(value, stretch - W + 1 - e, 1)[:, 0:cells]
            below = below if e == 1 else below * keep[e][:, 0:cells]
            shifted[e][f, ch : ch + 16, stretch : stretch + cells] = below

    def pack(i):
        at = pl.multiple_of(i * 16, 16)
        for a in range(3):
            taps = [[w2[a, b, e, pl.ds(at, 16), :].astype(F32) for e in range(3)] for b in range(3)]
            for py in range(2):
                if py == 0:
                    pair_of_lines = (taps[0], [taps[1][e] + taps[2][e] for e in range(3)])
                else:
                    pair_of_lines = ([taps[0][e] + taps[1][e] for e in range(3)], taps[2])
                for px in range(2):
                    for iy, taken in enumerate(pair_of_lines):
                        if px == 0:
                            pair = (taken[0], taken[1] + taken[2])
                        else:
                            pair = (taken[0] + taken[1], taken[2])
                        for ix, value in enumerate(pair):
                            start = ((a * 2 + iy) * 2 + ix) * mid
                            packed[2 * py + px, pl.ds(at, 16), start : start + mid] = value.astype(BF16)

    lax.fori_loop(0, width // 16, lambda i, c: pack(i) or 0, 0)
    columns[0, 0:mid] = column_of(b1[...].reshape(1, mid), 128)
    columns[1, 0:mid] = column_of(gain[...].reshape(1, mid), 128)
    columns[2, 0:width] = column_of(b2[...].reshape(1, width), 128)

    for side in range(2):

        @pl.when(jnp.logical_not(has[side]))
        def _clear():
            edges[side] = jnp.zeros(edges.shape[1:], BF16)

        @pl.when(has[side])
        def _arrive():
            for copy in edge_copies(1 - side):
                copy.wait_recv()

    for f in range(history):
        sides = [jnp.where(has[i], halo[i, f], jnp.zeros((), BF16)) for i in range(2)]
        tall = jnp.concatenate([sides[0], feature_cache[f].reshape(cells, mid), sides[1]], axis=0)
        pre[...] = jnp.transpose(tall.astype(F32))
        for ch in range(0, mid, 16):
            spread(f, pre[ch : ch + 16, :], ch)

    def convolve(t, phase, taken):
        py, px = phase // 2, phase % 2
        parts = []
        for a in taken:
            for iy in range(2):
                begin = (0, stretch, 2 * W)[py + iy]
                for ix in range(2):
                    parts.append(shifted[px + ix][t + a, :, begin : begin + cells])
        begin, end = taken[0] * 4 * mid, (taken[-1] + 1) * 4 * mid
        return jnp.dot(
            packed[phase, :, begin:end], jnp.concatenate(parts, axis=0), preferred_element_type=F32
        )

    for t in range(history):
        for phase in range(4):
            partial[t, phase] = convolve(t, phase, range(history - t))

    def arrive(i):
        peer = lax.rem(me + 1 + i, devices)
        pltpu.make_async_remote_copy(
            src_ref=outgoing.at[0],
            dst_ref=incoming.at[peer],
            send_sem=send_sem.at[peer],
            recv_sem=recv_sem.at[peer],
            device_id={"seq": peer},
        ).wait_recv()

    trips(devices - 1, arrive)

    def place(i, total):
        pieces = []
        for half in range(2):
            got = incoming[2 * i + half]
            pieces.append(jnp.concatenate([got] * lines, axis=0) * line_mask[2 * i + half])
        hot = column_hot[pl.ds(pl.multiple_of(i * 256, 256), 256)]
        return total + jnp.dot(jnp.concatenate(pieces, axis=1), hot, preferred_element_type=F32)

    pairs = devices // 2
    placed = lax.fori_loop(
        0,
        pairs,
        place,
        jnp.zeros((lines * LAT_CH, 128), F32),
        unroll=True if pairs <= 16 else 1,
    )
    left = lane_index((LAT_CH, 128)) < W
    block = (inner + 4) * W
    for i in range(lines // 2):
        low = placed[2 * i * LAT_CH : (2 * i + 1) * LAT_CH]
        high = placed[(2 * i + 1) * LAT_CH : (2 * i + 2) * LAT_CH]
        start = history * block + i * 128
        first[:, start : start + 128] = jnp.where(left, low, high).astype(BF16)
    for f in range(history):
        first[:, f * block : f * block + 128] = edges[0, f]
        for r in range(inner // 2):
            start = f * block + 128 + r * 128
            first[:, start : start + 128] = past[f, r]
        first[:, f * block + block - 128 : f * block + block] = edges[1, f]

    value = first[...].astype(F32)
    total = value.shape[1]
    col = lane_index(value.shape) % W
    left = jnp.where(col == 0, 0.0, pltpu.roll(value, 1, 1))
    right = jnp.where(col == W - 1, 0.0, pltpu.roll(value, total - 1, 1))
    shifts = [v.astype(BF16) for v in (left, value, right)]
    later = [pltpu.roll(v, total - W, 1).astype(BF16) for v in (left, value, right)]
    row = lane_index((16, stretch)) // W
    outside = ((row == 0) & jnp.logical_not(has[0])) | ((row == high_rows - 1) & jnp.logical_not(has[1]))
    bias = jnp.concatenate([columns[2, 0:width]] * (cells // 128), axis=1)
    for t in range(FMAX):
        patch = []
        for a in range(3):
            for b in range(3):
                source, begin = (later, 0) if b == 1 else (shifts, b * W)
                begin += (t + a) * block
                for e in range(3):
                    patch.append(source[e][:, begin : begin + stretch])
        pre[...] = lax.dot_general(
            w1[...].reshape(27 * LAT_CH, mid),
            jnp.concatenate(patch, axis=0),
            (((0,), (0,)), ((), ())),
            preferred_element_type=F32,
        )
        squares = jnp.zeros((16, stretch), F32)
        for ch in range(0, mid, 16):
            x = pre[ch : ch + 16, :]
            x = x + jnp.concatenate([columns[0, ch : ch + 16]] * (stretch // 128), axis=1)
            pre[ch : ch + 16, :] = x
            squares = squares + x * x
        inverse = lax.rsqrt(jnp.sum(squares, axis=0, keepdims=True) / mid + 1e-06)
        for ch in range(0, mid, 16):
            scale = jnp.concatenate([columns[1, ch : ch + 16]] * (stretch // 128), axis=1)
            x = pre[ch : ch + 16, :] * inverse * scale
            x = x / (1.0 + jnp.exp(-x))
            spread(history + t, jnp.where(outside, 0.0, x), ch)
        for phase in range(4):
            result = convolve(t, phase, range(max(history - t, 0), 3))
            if t < history:
                result = result + partial[t, phase]
            halves[t, phase] = (result + bias).astype(BF16)

    trips(devices - 1, lambda i: copy_to(i).wait_send())
    for side in range(2):

        @pl.when(has[side])
        def _sent():
            for copy in edge_copies(side):
                copy.wait_send()


def finish_kernel(
    assign_hbm,
    counts_hbm,
    halves,
    center,
    first,
    out,
    carry,
    latent_next,
    assign,
    counts,
    out_buf,
    carry_buf,
    latent_buf,
    load_sem,
    sems,
):
    loads = [
        pltpu.make_async_copy(assign_hbm, assign, load_sem.at[0]),
        pltpu.make_async_copy(counts_hbm, counts, load_sem.at[1]),
    ]
    for load in loads:
        load.start()
    frames, _, width, cells = halves.shape
    history, inner, _, mid = carry.shape
    devices = lax.axis_size("seq")
    group, _ = place_of(lax.axis_index("seq"), devices, devices // REQS)
    pair = 2 * W
    stores = []

    def store(source, target):
        copy = pltpu.make_async_copy(source, target, sems.at[len(stores)])
        copy.start()
        stores.append(copy)

    spot = sublane_index((2 * pair, 2 * pair))
    goal = spot // pair + 2 * (spot % pair)
    mix = (lane_index((2 * pair, 2 * pair)) == goal).astype(BF16)
    for t in range(frames):
        if t == 1:
            for load in loads:
                load.wait()
            count = counts[assign[group]]
        for i in range(0, inner, 2):
            for py in range(2):
                both = jnp.concatenate(
                    [halves[t, 2 * py + px, :, i * W : i * W + pair] for px in range(2)], axis=1
                )
                mixed = jnp.dot(both, mix, preferred_element_type=F32).astype(BF16)
                if t > 0:
                    mixed = jnp.where(t < count, mixed, jnp.zeros((), BF16))
                out_buf[t, 2 * i + py] = mixed[:, 0:pair]
                out_buf[t, 2 * i + 2 + py] = mixed[:, pair : 2 * pair]
        store(out_buf.at[t], out.at[t])
    for i in range(history):
        turned = jnp.transpose(center[count + i, :, (inner + 2) * W :].astype(F32)).astype(BF16)
        carry_buf[i] = turned.reshape(inner, W, mid)
    store(carry_buf, carry)
    parts = []
    for i in range(history):
        start = pl.multiple_of((count + i) * (inner + 4) * W + 2 * W, 128)
        own = first[:, pl.ds(start, cells)].astype(F32)
        for r in range(inner):
            parts.append(own[:, r * W : (r + 1) * W])
    stacked = jnp.concatenate(parts, axis=0).astype(BF16)
    shape = (W, W * LAT_CH)
    pick = sublane_index(shape) == lane_index(shape) // LAT_CH
    wide = jnp.dot(stacked, pick.astype(BF16), preferred_element_type=F32)
    wide = wide.reshape(history * inner, LAT_CH, W * LAT_CH)
    mine = sublane_index(wide.shape) == lane_index(wide.shape) % LAT_CH
    latent_buf[...] = (
        jnp.sum(jnp.where(mine, wide, 0.0), axis=1).astype(BF16).reshape(history, inner, W * LAT_CH)
    )
    store(latent_buf, latent_next)
    for copy in stores:
        copy.wait()


def section(assign, counts, latents, layout, latent_cache, feature_cache, w1, b1, gain, w2, b2):
    devices, slots = layout.shape
    history, inner, _, mid = feature_cache.shape
    width = b2.shape[0]
    per_group = devices // REQS
    windows = REQS * (per_group - min(3, per_group) + 1)
    lines = FMAX * (inner + 4)
    cells = inner * W
    stretch = (inner + 2) * W
    vmem = pl.BlockSpec(memory_space=pltpu.VMEM)
    hbm = pl.BlockSpec(memory_space=pltpu.HBM)
    inputs = (assign, latents, layout, latent_cache, feature_cache, w1, b1, gain, w2, b2)
    halves, center, first = pl.pallas_call(
        functools.partial(section_kernel, devices),
        in_specs=[hbm] * len(inputs),
        out_specs=[vmem] * 3,
        out_shape=[
            jax.ShapeDtypeStruct((FMAX, 4, width, cells), BF16),
            jax.ShapeDtypeStruct((history + FMAX, mid, stretch + cells), BF16),
            jax.ShapeDtypeStruct((LAT_CH, (history + FMAX) * (inner + 4) * W), BF16),
        ],
        scratch_shapes=[(pltpu.SMEM if i < 1 else pltpu.VMEM)(x.shape, x.dtype) for i, x in enumerate(inputs)]
        + [
            pltpu.VMEM((2, history, W, mid), BF16),
            pltpu.VMEM((windows, LAT_CH, 128), BF16),
            pltpu.VMEM((devices, LAT_CH, 128), BF16),
            pltpu.VMEM((history, inner // 2, LAT_CH, 128), BF16),
            pltpu.VMEM((2, history, LAT_CH, 128), BF16),
            pltpu.VMEM((devices, slots), F32),
            pltpu.VMEM((devices, slots), F32),
            pltpu.VMEM((max(devices, windows), slots), F32),
            pltpu.VMEM((devices, lines * LAT_CH, 128), BF16),
            pltpu.VMEM((devices * 128, 128), BF16),
            pltpu.VMEM((2, history + FMAX, mid, stretch + cells), BF16),
            pltpu.VMEM((4, width, 12 * mid), BF16),
            pltpu.VMEM((history, 4, width, cells), F32),
            pltpu.VMEM((mid, stretch), F32),
            pltpu.VMEM((3, mid, 128), F32),
            pltpu.SemaphoreType.DMA((len(inputs),)),
            pltpu.SemaphoreType.DMA((devices,)),
            pltpu.SemaphoreType.DMA((devices,)),
            pltpu.SemaphoreType.DMA((2, history)),
            pltpu.SemaphoreType.DMA((2, history)),
            pltpu.SemaphoreType.DMA((2, history)),
            pltpu.SemaphoreType.DMA((2, history)),
        ],
        compiler_params=pltpu.CompilerParams(
            collective_id=0, has_side_effects=True, vmem_limit_bytes=44 * 1024 * 1024
        ),
    )(*[in_hbm(x) for x in inputs])
    return pl.pallas_call(
        finish_kernel,
        in_specs=[hbm] * 2 + [vmem] * 3,
        out_specs=[hbm] * 3,
        out_shape=[
            jax.ShapeDtypeStruct((FMAX, 2 * inner, width, 2 * W), BF16),
            jax.ShapeDtypeStruct((history, inner, W, mid), BF16),
            jax.ShapeDtypeStruct((history, inner, W * LAT_CH), BF16),
        ],
        scratch_shapes=[
            pltpu.SMEM(assign.shape, assign.dtype),
            pltpu.SMEM(counts.shape, counts.dtype),
            pltpu.VMEM((FMAX, 2 * inner, width, 2 * W), BF16),
            pltpu.VMEM((history, inner, W, mid), BF16),
            pltpu.VMEM((history, inner, W * LAT_CH), BF16),
            pltpu.SemaphoreType.DMA((2,)),
            pltpu.SemaphoreType.DMA((FMAX + 2,)),
        ],
        compiler_params=pltpu.CompilerParams(vmem_limit_bytes=16 * 1024 * 1024),
    )(in_hbm(assign), in_hbm(counts), halves, center, first)


def body(
    latents,
    layout,
    assign,
    counts,
    latent_cache,
    feature_cache,
    first_weight,
    first_bias,
    norm_gain,
    second_weight,
    second_bias,
):
    decoded_frames, feature_next, latent_next = section(
        assign,
        counts,
        latents,
        layout,
        latent_cache,
        feature_cache,
        first_weight,
        first_bias,
        norm_gain,
        jnp.swapaxes(second_weight, 3, 4),
        second_bias,
    )
    return (jnp.swapaxes(decoded_frames, 2, 3), latent_next, feature_next)


def solution(mesh):
    return jax.shard_map(
        body,
        mesh=mesh,
        in_specs=(
            P(None, ("rep", "seq")),
            P("rep", None),
            P("rep"),
            P("rep"),
            P(None, ("rep", "seq"), None),
            P(None, ("rep", "seq"), None, None),
            P(),
            P(),
            P(),
            P(),
            P(),
        ),
        out_specs=(
            P(None, ("rep", "seq"), None, None),
            P(None, ("rep", "seq"), None),
            P(None, ("rep", "seq"), None, None),
        ),
        check_vma=False,
    )
```

```python
import functools

import jax
import jax.numpy as jnp
from jax import lax
from jax.experimental import pallas as pl
from jax.experimental.pallas import tpu as pltpu
from jax.sharding import PartitionSpec as P

LAT_CH = 16
REQS = 8
FMAX = 3
ROWS_DEV = 4
W = 64
F32 = jnp.float32
BF16 = jnp.bfloat16


def lane_index(shape):
    return lax.broadcasted_iota(jnp.int32, shape, len(shape) - 1)


def in_hbm(array):
    return pltpu.with_memory_space_constraint(array, pltpu.HBM)


def column_of(row, lanes):
    return jnp.transpose(jnp.broadcast_to(row, (lanes, row.shape[1])))


def sublane_index(shape):
    return lax.broadcasted_iota(jnp.int32, shape, len(shape) - 2)


def trips(count, step, carry=None):
    body = lambda i, c: step(i) or 0
    lax.fori_loop(0, count, body, 0, unroll=True if count <= 16 else 1)


def ranks_in(mask, before):
    rows, slots = mask.shape
    blocks = slots // 128
    stacked = jnp.concatenate([mask[:, i * 128 : i * 128 + 128] for i in range(blocks)], axis=0)
    counted = jnp.dot(stacked.astype(BF16), before, preferred_element_type=F32)
    base = jnp.zeros((rows, 128), F32)
    ranks = []
    for i in range(blocks):
        block = counted[i * rows : (i + 1) * rows]
        ranks.append(block[:, 0:128] + base)
        base = base + block[:, 128:256]
    return jnp.where(mask > 0.0, jnp.concatenate(ranks, axis=1), -1.0)


def peer_of(me, i, devices):
    if devices & (devices - 1):
        return lax.rem(me + 1 + i, devices)
    return me ^ (devices - 1 - i)


def place_of(device, devices, per_group):
    place = lax.rem(device + per_group // 2, devices)
    return place // per_group, lax.rem(place, per_group)


def section_kernel(
    devices,
    assign_hbm,
    counts_hbm,
    latents_hbm,
    layout_hbm,
    latent_cache_hbm,
    feature_cache_hbm,
    w1_hbm,
    b1_hbm,
    gain_hbm,
    w2_hbm,
    b2_hbm,
    frames_out,
    center,
    first,
    live,
    assign,
    counts,
    latents,
    layout,
    latent_cache,
    feature_cache,
    w1,
    b1,
    gain,
    w2,
    b2,
    halo,
    outgoing,
    incoming,
    past,
    edges,
    row_line,
    row_column,
    row_rank,
    line_mask,
    column_hot,
    feat,
    packed,
    partial,
    pre,
    turn,
    mix,
    columns,
    load_sem,
    send_sem,
    recv_sem,
    edge_send,
    edge_recv,
    halo_send,
    halo_recv,
):
    me = lax.axis_index("seq")
    per_group = devices // REQS
    slots = layout.shape[1]
    history, inner, wide = latent_cache.shape
    height = inner * per_group
    span = min(3, per_group)
    starts = per_group - span + 1
    used = -(-span * (slots // devices) // 16) * 16
    lines = FMAX * (inner + 4)
    group, position = place_of(me, devices, per_group)
    above = lax.rem(me + devices - 1, devices)
    below = lax.rem(me + 1, devices)

    barrier = pltpu.get_barrier_semaphore()

    def greet(i):
        pl.semaphore_signal(barrier, inc=1, device_id={"seq": peer_of(me, i, devices)})

    trips(devices - 1, greet)

    loads = [
        pltpu.make_async_copy(source, target, load_sem.at[i])
        for i, (source, target) in enumerate(
            (
                (assign_hbm, assign),
                (layout_hbm, layout),
                (latents_hbm, latents),
                (latent_cache_hbm, latent_cache),
                (counts_hbm, counts),
                (feature_cache_hbm, feature_cache),
                (w2_hbm, w2),
                (w1_hbm, w1),
                (b1_hbm, b1),
                (gain_hbm, gain),
                (b2_hbm, b2),
            )
        )
    ]
    for load in loads:
        load.start()


    for load in loads[0:4]:
        load.wait()

    for f in range(history):
        stacked = []
        for r in range(inner):
            row = jnp.broadcast_to(latent_cache[f, r : r + 1, :].astype(F32), (LAT_CH, wide))
            mine = sublane_index(row.shape) == lane_index(row.shape) % LAT_CH
            stacked.append(jnp.where(mine, row, 0.0).astype(BF16))
        pick = sublane_index((wide, 128)) // LAT_CH == lane_index((wide, 128)) % W
        turned = jnp.dot(
            jnp.concatenate(stacked, axis=0), pick.astype(BF16), preferred_element_type=F32
        ).astype(BF16)
        for r in range(0, inner, 2):
            low = turned[r * LAT_CH : (r + 1) * LAT_CH]
            high = turned[(r + 1) * LAT_CH : (r + 2) * LAT_CH]
            left = lane_index(low.shape) < W
            past[f, r // 2] = jnp.where(left, low, high)

    square = (128, 256)
    earlier = (sublane_index(square) < lane_index(square)) | (lane_index(square) >= 128)
    before = earlier.astype(BF16)
    mine = layout[pl.ds(me, 1), :]
    remain = mine // W
    row = lax.rem(remain, height)
    step = remain // height
    windows = REQS * starts
    window = sublane_index((windows, slots))
    request = jnp.zeros((windows, slots), jnp.int32)
    for g in range(REQS):
        request = jnp.where(window // starts == g, assign[g], request)
    low = lax.rem(window, starts) * inner
    member = (step >= request * FMAX) & (step < request * FMAX + FMAX)
    member = member & (row >= low) & (row < low + span * inner)
    rank = ranks_in(jnp.where(member, 1.0, 0.0), before)
    row_rank[0:windows] = rank

    def chosen(i):
        ranked = row_rank[pl.ds(i, 1), :]
        hot = sublane_index((used, slots)).astype(F32) == ranked
        hot = jnp.where(hot, 1.0, 0.0).astype(BF16)
        if used < 128:
            hot = jnp.concatenate([hot, jnp.zeros((128 - used, slots), BF16)], axis=0)
        return hot

    def collect(i):
        hot = jnp.concatenate([chosen(2 * i), chosen(2 * i + 1)], axis=0)
        moved = lax.dot_general(
            latents[...], hot, (((1,), (1,)), ((), ())), preferred_element_type=F32
        ).astype(BF16)
        outgoing[2 * i] = moved[:, 0:128]
        outgoing[2 * i + 1] = moved[:, 128:256]

    trips(windows // 2, collect)

    pl.semaphore_wait(barrier, devices - 1)

    def window_of(device):
        g, k = place_of(device, devices, per_group)
        return g * starts + jnp.clip(k - 1, 0, starts - 1)

    def copy_to(i):
        peer = peer_of(me, i, devices)
        return pltpu.make_async_remote_copy(
            src_ref=outgoing.at[window_of(peer)],
            dst_ref=incoming.at[me],
            send_sem=send_sem.at[peer],
            recv_sem=recv_sem.at[me],
            device_id={"seq": peer},
        )

    trips(devices - 1, lambda i: copy_to(i).start())

    def edge_copies(side):
        peer = (above, below)[side]
        copies = []
        for f in range(history):
            copies.append(
                pltpu.make_async_remote_copy(
                    src_ref=past.at[f, 0 if side == 0 else inner // 2 - 1],
                    dst_ref=edges.at[1 - side, f],
                    send_sem=edge_send.at[side, f],
                    recv_sem=edge_recv.at[1 - side, f],
                    device_id={"seq": peer},
                )
            )
            copies.append(
                pltpu.make_async_remote_copy(
                    src_ref=feature_cache.at[f, 0 if side == 0 else inner - 1],
                    dst_ref=halo.at[1 - side, f],
                    send_sem=halo_send.at[side, f],
                    recv_sem=halo_recv.at[1 - side, f],
                    device_id={"seq": peer},
                )
            )
        return copies

    has = (position > 0, position < per_group - 1)
    for load in loads[4:6]:
        load.wait()
    for side in range(2):

        @pl.when(has[side])
        def _start():
            for copy in edge_copies(side):
                copy.start()

    incoming[me] = outgoing[window_of(me)]

    number = layout[...]
    remain = number // W
    row = lax.rem(remain, height)
    step = remain // height - assign[group] * FMAX
    first_tile = jnp.clip(position - 1, 0, starts - 1)
    member = (step >= 0) & (step < FMAX)
    member = member & (row >= first_tile * inner) & (row < (first_tile + span) * inner)
    rank = ranks_in(jnp.where(member, 1.0, 0.0), before)
    local = row - (position * inner - 2)
    line = jnp.where((local >= 0) & (local < inner + 4), step * (inner + 4) + local + 1, 0)
    row_rank[0:devices] = rank
    row_line[...] = line.astype(F32)
    row_column[...] = lax.rem(number, W).astype(F32)

    def locate(i):
        ranked = row_rank[pl.ds(i, 1), :]
        hot = sublane_index((128, slots)).astype(F32) == ranked
        hot = jnp.where(hot, 1.0, 0.0).astype(BF16)
        shape = (16, slots)
        what = jnp.where(
            sublane_index(shape) == 0, row_line[pl.ds(i, 1), :], row_column[pl.ds(i, 1), :]
        ).astype(BF16)
        found = lax.dot_general(what, hot, (((1,), (1,)), ((), ())), preferred_element_type=F32)
        level = sublane_index((lines * LAT_CH, 128)) // LAT_CH + 1
        line_mask[i] = jnp.where(level.astype(F32) == found[0:1], 1.0, 0.0).astype(BF16)
        column = jnp.transpose(jnp.broadcast_to(found[1:2], (128, 128)))
        same = column == (lane_index((128, 128)) % W).astype(F32)
        column_hot[pl.ds(pl.multiple_of(i * 128, 128), 128)] = jnp.where(same, 1.0, 0.0).astype(BF16)

    trips(devices, locate)

    mid = feature_cache.shape[3]
    width = b2.shape[0]
    cells = inner * W
    stretch = (inner + 2) * W
    shifted = (feat.at[0], center, feat.at[1])

    def edge_mask(lanes):
        col = lane_index((16, lanes)) % W
        return ((col != 0).astype(BF16), None, (col != W - 1).astype(BF16))

    keep = edge_mask(stretch)

    def spread(f, value, ch):
        for e in range(3):
            moved = value if e == 1 else pltpu.roll(value, (1, 0, stretch - 1)[e], 1) * keep[e]
            shifted[e][f, ch : ch + 16, 0:stretch] = moved

    def spread_inner(f, value, ch):
        for e in range(3):
            moved = value if e == 1 else pltpu.roll(value, (1, 0, cells - 1)[e], 1) * keep[e][:, 0:cells]
            shifted[e][f, ch : ch + 16, stretch : stretch + cells] = moved

    def pack(i):
        at = pl.multiple_of(i * 16, 16)
        for a in range(3):
            taps = [[w2[a, b, e, pl.ds(at, 16), :] for e in range(3)] for b in range(3)]
            add = lambda r, e, q, d: taps[r][e] + taps[q][d]
            for py in range(2):
                edge = 2 * py
                top, low = (1, 2) if py == 0 else (0, 1)
                both = [taps[top][e].astype(F32) + taps[low][e].astype(F32) for e in range(3)]
                for px in range(2):
                    one, near, far = (0, 1, 2) if px == 0 else (2, 0, 1)
                    values = (
                        (add(top, one, low, one), both[near] + both[far]),
                        (taps[edge][one], add(edge, near, edge, far)),
                    )
                    for side in range(2):
                        for which in range(2):
                            ix = which if px == 0 else 1 - which
                            start = ((side * 3 + a) * 2 + ix) * mid
                            packed[2 * py + px, pl.ds(at, 16), start : start + mid] = values[side][which].astype(BF16)

    for load in loads[6:]:
        load.wait()
    lax.fori_loop(0, width // 16, lambda i, c: pack(i) or 0, 0)
    columns[0, 0:mid] = column_of(b1[...].reshape(1, mid), 128)
    columns[1, 0:mid] = column_of(gain[...].reshape(1, mid), 128)
    columns[2, 0:width] = column_of(b2[...].reshape(1, width), 128)
    pair = 2 * W
    spot = sublane_index((2 * pair, 2 * pair))
    goal = spot // pair + 2 * (spot % pair)
    mix[...] = (lane_index((2 * pair, 2 * pair)) == goal).astype(BF16)
    request = assign[group]
    count = jnp.int32(0)
    for r in range(REQS):
        count = count + jnp.where(request == r, counts[r], 0)
    live[...] = jnp.full(live.shape, count, jnp.int32)

    for f in range(history):
        pre[:, 0:cells] = jnp.transpose(feature_cache[f].reshape(cells, mid).astype(F32))
        for ch in range(0, mid, 16):
            spread_inner(f, pre[ch : ch + 16, 0:cells].astype(BF16), ch)

    def convolve(t, phase, pieces):
        py, px = phase // 2, phase % 2
        total = None
        for side, first_a, last_a in pieces:
            parts = []
            for a in range(first_a, last_a):
                for ix in range(2):
                    begin = stretch if side == 0 else (0 if py == 0 else 2 * W)
                    parts.append(shifted[px + ix][t + a, :, begin : begin + cells])
            begin, end = (side * 3 + first_a) * 2 * mid, (side * 3 + last_a) * 2 * mid
            product = jnp.dot(
                packed[phase, :, begin:end], jnp.concatenate(parts, axis=0), preferred_element_type=F32
            )
            total = product if total is None else total + product
        return total

    for t in range(history):
        for phase in range(4):
            partial[t, phase] = convolve(t, phase, ((0, 0, history - t),))

    for side in range(2):

        @pl.when(jnp.logical_not(has[side]))
        def _clear():
            edges[side] = jnp.zeros(edges.shape[1:], BF16)

        @pl.when(has[side])
        def _arrive():
            for copy in edge_copies(1 - side)[0::2]:
                copy.wait_recv()

    def arrive(i):
        peer = peer_of(me, i, devices)
        pltpu.make_async_remote_copy(
            src_ref=outgoing.at[0],
            dst_ref=incoming.at[peer],
            send_sem=send_sem.at[peer],
            recv_sem=recv_sem.at[peer],
            device_id={"seq": peer},
        ).wait_recv()

    trips(devices - 1, arrive)

    def place(i, total):
        pieces = []
        for half in range(2):
            got = incoming[2 * i + half]
            pieces.append(jnp.concatenate([got] * lines, axis=0) * line_mask[2 * i + half])
        hot = column_hot[pl.ds(pl.multiple_of(i * 256, 256), 256)]
        return total + jnp.dot(jnp.concatenate(pieces, axis=1), hot, preferred_element_type=F32)

    pairs = devices // 2
    placed = lax.fori_loop(
        0,
        pairs,
        place,
        jnp.zeros((lines * LAT_CH, 128), F32),
        unroll=True if pairs <= 16 else 1,
    )
    left = lane_index((LAT_CH, 128)) < W
    block = (inner + 4) * W
    for i in range(lines // 2):
        low = placed[2 * i * LAT_CH : (2 * i + 1) * LAT_CH]
        high = placed[(2 * i + 1) * LAT_CH : (2 * i + 2) * LAT_CH]
        start = history * block + i * 128
        first[:, start : start + 128] = jnp.where(left, low, high).astype(BF16)
    for f in range(history):
        first[:, f * block : f * block + 128] = edges[0, f]
        for r in range(inner // 2):
            start = f * block + 128 + r * 128
            first[:, start : start + 128] = past[f, r]
        first[:, f * block + block - 128 : f * block + block] = edges[1, f]

    value = first[...].astype(F32)
    total = value.shape[1]
    col = lane_index(value.shape) % W
    left = jnp.where(col == 0, 0.0, pltpu.roll(value, 1, 1))
    right = jnp.where(col == W - 1, 0.0, pltpu.roll(value, total - 1, 1))
    shifts = [v.astype(BF16) for v in (left, value, right)]
    later = [pltpu.roll(v, total - W, 1).astype(BF16) for v in (left, value, right)]
    row = lane_index((16, stretch)) // W
    outside = (row == 0) & jnp.logical_not(has[0])
    outside = outside | ((row == inner + 1) & jnp.logical_not(has[1]))
    inside = jnp.where(outside, 0.0, 0.5)
    bias = jnp.concatenate([columns[2, 0:width]] * (cells // 128), axis=1)
    patches = []
    for a in range(3):
        for b in range(3):
            for e in range(3):
                source = later[e] if b == 1 else shifts[e]
                begin = a * block + (0 if b == 1 else b * W)
                patches.append(
                    jnp.concatenate(
                        [source[:, begin + t * block : begin + t * block + stretch] for t in range(FMAX)],
                        axis=1,
                    )
                )
    pre[...] = lax.dot_general(
        w1[...].reshape(27 * LAT_CH, mid),
        jnp.concatenate(patches, axis=0),
        (((0,), (0,)), ((), ())),
        preferred_element_type=F32,
    )
    repeat = lambda x: jnp.concatenate([x] * (stretch // 128), axis=1)
    biased = lambda t, ch: pre[ch : ch + 16, t * stretch : (t + 1) * stretch] + repeat(
        columns[0, ch : ch + 16]
    )

    def norms(t):
        squares = jnp.zeros((16, stretch), F32)
        for ch in range(0, mid, 16):
            x = biased(t, ch)
            squares = squares + x * x
        inverse = lax.rsqrt(jnp.sum(squares, axis=0, keepdims=True) / mid + 1e-06)
        return jnp.broadcast_to(inverse, (16, stretch))

    def activate(t, inverse, chs):
        for ch in chs:
            x = biased(t, ch) * inverse * repeat(columns[1, ch : ch + 16])
            y = x * inside
            y = (y + y * jnp.tanh(0.5 * x)).astype(BF16)
            spread(history + t, y, ch)
            own = pltpu.roll(y, stretch - W, 1)[:, 0:cells]
            spread_inner(history + t, own, ch)

    steps = list(range(0, mid, 16))
    activate(0, norms(0), steps)
    alive = live[0:1, :]
    def emit(t, pieces):
        shown = jnp.broadcast_to(alive, (width, pair)) > t
        held = []
        for phase in range(4):
            result = convolve(t, phase, pieces)
            if t < history:
                result = result + partial[t, phase]
            held.append((result + bias).astype(BF16))
            if phase % 2 == 0:
                continue
            for i in range(0, inner, 2):
                both = jnp.concatenate([half[:, i * W : i * W + pair] for half in held], axis=1)
                mixed = jnp.dot(both, mix[...], preferred_element_type=F32)
                for j in range(2):
                    kept = jnp.where(shown, mixed[:, j * pair : (j + 1) * pair], 0.0)
                    frames_out[t, 2 * (i + j) + phase // 2] = kept.astype(BF16)
            held = []

    for t in range(FMAX):
        if t < history:
            following = norms(t + 1)
            for phase in range(4):
                fresh = convolve(t, phase, ((0, history - t, 3), (1, history - t, 3)))
                partial[t, phase] = partial[t, phase] + fresh
                activate(t + 1, following, steps[phase * len(steps) // 4 : (phase + 1) * len(steps) // 4])
        else:
            emit(t, ((0, 0, 3), (1, 0, 3)))
    for side in range(2):

        @pl.when(has[side])
        def _halo():
            for copy in edge_copies(1 - side)[1::2]:
                copy.wait_recv()

    for f in range(history):
        sides = [jnp.where(has[i], halo[i, f], jnp.zeros((), BF16)) for i in range(2)]
        tall = jnp.concatenate([sides[0], feature_cache[f].reshape(cells, mid), sides[1]], axis=0)
        turn[:, 0:stretch] = jnp.transpose(tall.astype(F32))
        for ch in range(0, mid, 16):
            spread(f, turn[ch : ch + 16, 0:stretch].astype(BF16), ch)

    for t in range(history):
        emit(t, ((1, 0, history - t),))

    trips(devices - 1, lambda i: copy_to(i).wait_send())
    for side in range(2):

        @pl.when(has[side])
        def _sent():
            for copy in edge_copies(side):
                copy.wait_send()


def finish_kernel(frames, center, first, live, out, carry, latent_next, carry_buf, latent_buf, sems):
    history, inner, _, mid = carry.shape
    cells = inner * W
    block = (inner + 4) * W
    stores = []

    def store(source, target):
        copy = pltpu.make_async_copy(source, target, sems.at[len(stores)])
        copy.start()
        stores.append(copy)

    for t in range(FMAX):
        store(frames.at[t], out.at[t])

    def picked(values):
        count = jnp.broadcast_to(live[0:1, 0:1], values[0].shape)
        result = values[0]
        for n in range(1, FMAX):
            result = jnp.where(count == n + 1, values[n], result)
        return result

    for i in range(history):
        begin = (inner + 2) * W
        choice = [center[1 + n + i, :, begin : begin + cells].astype(F32) for n in range(FMAX)]
        carry_buf[i] = jnp.transpose(picked(choice)).astype(BF16).reshape(inner, W, mid)
    store(carry_buf, carry)
    parts = []
    for i in range(history):
        start = (1 + i) * block + 2 * W
        choice = [first[:, start + n * block : start + n * block + cells].astype(F32) for n in range(FMAX)]
        own = picked(choice)
        for r in range(inner):
            parts.append(own[:, r * W : (r + 1) * W])
    stacked = jnp.concatenate(parts, axis=0).astype(BF16)
    shape = (W, W * LAT_CH)
    pick = sublane_index(shape) == lane_index(shape) // LAT_CH
    wide = jnp.dot(stacked, pick.astype(BF16), preferred_element_type=F32)
    wide = wide.reshape(history * inner, LAT_CH, W * LAT_CH)
    mine = sublane_index(wide.shape) == lane_index(wide.shape) % LAT_CH
    latent_buf[...] = (
        jnp.sum(jnp.where(mine, wide, 0.0), axis=1).astype(BF16).reshape(history, inner, W * LAT_CH)
    )
    store(latent_buf, latent_next)
    for copy in stores:
        copy.wait()


def section(assign, counts, latents, layout, latent_cache, feature_cache, w1, b1, gain, w2, b2):
    devices, slots = layout.shape
    history, inner, _, mid = feature_cache.shape
    width = b2.shape[0]
    per_group = devices // REQS
    windows = REQS * (per_group - min(3, per_group) + 1)
    lines = FMAX * (inner + 4)
    cells = inner * W
    stretch = (inner + 2) * W
    vmem = pl.BlockSpec(memory_space=pltpu.VMEM)
    hbm = pl.BlockSpec(memory_space=pltpu.HBM)
    inputs = (assign, counts, latents, layout, latent_cache, feature_cache, w1, b1, gain, w2, b2)
    frames, center, first, live = pl.pallas_call(
        functools.partial(section_kernel, devices),
        in_specs=[hbm] * len(inputs),
        out_specs=[vmem] * 4,
        out_shape=[
            jax.ShapeDtypeStruct((FMAX, 2 * inner, width, 2 * W), BF16),
            jax.ShapeDtypeStruct((history + FMAX, mid, stretch + cells), BF16),
            jax.ShapeDtypeStruct((LAT_CH, (history + FMAX) * (inner + 4) * W), BF16),
            jax.ShapeDtypeStruct((8, 128), jnp.int32),
        ],
        scratch_shapes=[(pltpu.SMEM if i < 2 else pltpu.VMEM)(x.shape, x.dtype) for i, x in enumerate(inputs)]
        + [
            pltpu.VMEM((2, history, W, mid), BF16),
            pltpu.VMEM((windows, LAT_CH, 128), BF16),
            pltpu.VMEM((devices, LAT_CH, 128), BF16),
            pltpu.VMEM((history, inner // 2, LAT_CH, 128), BF16),
            pltpu.VMEM((2, history, LAT_CH, 128), BF16),
            pltpu.VMEM((devices, slots), F32),
            pltpu.VMEM((devices, slots), F32),
            pltpu.VMEM((max(devices, windows), slots), F32),
            pltpu.VMEM((devices, lines * LAT_CH, 128), BF16),
            pltpu.VMEM((devices * 128, 128), BF16),
            pltpu.VMEM((2, history + FMAX, mid, stretch + cells), BF16),
            pltpu.VMEM((4, width, 12 * mid), BF16),
            pltpu.VMEM((history, 4, width, cells), F32),
            pltpu.VMEM((mid, FMAX * stretch), F32),
            pltpu.VMEM((mid, stretch), F32),
            pltpu.VMEM((4 * W, 4 * W), BF16),
            pltpu.VMEM((3, mid, 128), F32),
            pltpu.SemaphoreType.DMA((len(inputs),)),
            pltpu.SemaphoreType.DMA((devices,)),
            pltpu.SemaphoreType.DMA((devices,)),
            pltpu.SemaphoreType.DMA((2, history)),
            pltpu.SemaphoreType.DMA((2, history)),
            pltpu.SemaphoreType.DMA((2, history)),
            pltpu.SemaphoreType.DMA((2, history)),
        ],
        compiler_params=pltpu.CompilerParams(
            collective_id=0, has_side_effects=True, vmem_limit_bytes=44 * 1024 * 1024
        ),
    )(*[in_hbm(x) for x in inputs])
    return pl.pallas_call(
        finish_kernel,
        in_specs=[vmem] * 4,
        out_specs=[hbm] * 3,
        out_shape=[
            jax.ShapeDtypeStruct((FMAX, 2 * inner, width, 2 * W), BF16),
            jax.ShapeDtypeStruct((history, inner, W, mid), BF16),
            jax.ShapeDtypeStruct((history, inner, W * LAT_CH), BF16),
        ],
        scratch_shapes=[
            pltpu.VMEM((history, inner, W, mid), BF16),
            pltpu.VMEM((history, inner, W * LAT_CH), BF16),
            pltpu.SemaphoreType.DMA((FMAX + 2,)),
        ],
        compiler_params=pltpu.CompilerParams(vmem_limit_bytes=16 * 1024 * 1024),
    )(frames, center, first, live)


def body(
    latents,
    layout,
    assign,
    counts,
    latent_cache,
    feature_cache,
    first_weight,
    first_bias,
    norm_gain,
    second_weight,
    second_bias,
):
    decoded_frames, feature_next, latent_next = section(
        assign,
        counts,
        latents,
        layout,
        latent_cache,
        feature_cache,
        first_weight,
        first_bias,
        norm_gain,
        jnp.swapaxes(second_weight, 3, 4),
        second_bias,
    )
    return (jnp.swapaxes(decoded_frames, 2, 3), latent_next, feature_next)


def solution(mesh):
    return jax.shard_map(
        body,
        mesh=mesh,
        in_specs=(
            P(None, ("rep", "seq")),
            P("rep", None),
            P("rep"),
            P("rep"),
            P(None, ("rep", "seq"), None),
            P(None, ("rep", "seq"), None, None),
            P(),
            P(),
            P(),
            P(),
            P(),
        ),
        out_specs=(
            P(None, ("rep", "seq"), None, None),
            P(None, ("rep", "seq"), None),
            P(None, ("rep", "seq"), None, None),
        ),
        check_vma=False,
    )
```

```python
import functools

import jax
import jax.numpy as jnp
from jax import lax
from jax.experimental import pallas as pl
from jax.experimental.pallas import tpu as pltpu
from jax.sharding import PartitionSpec as P

LAT_CH = 16
REQS = 8
FMAX = 3
ROWS_DEV = 4
W = 64
F32 = jnp.float32
BF16 = jnp.bfloat16


def lane_index(shape):
    return lax.broadcasted_iota(jnp.int32, shape, len(shape) - 1)


def in_hbm(array):
    return pltpu.with_memory_space_constraint(array, pltpu.HBM)


def column_of(row, lanes):
    return jnp.transpose(jnp.broadcast_to(row, (lanes, row.shape[1])))


def sublane_index(shape):
    return lax.broadcasted_iota(jnp.int32, shape, len(shape) - 2)


def trips(count, step, carry=None):
    body = lambda i, c: step(i) or 0
    lax.fori_loop(0, count, body, 0, unroll=True if count <= 16 else 1)


def ranks_in(mask, before):
    rows, slots = mask.shape
    blocks = slots // 128
    stacked = jnp.concatenate([mask[:, i * 128 : i * 128 + 128] for i in range(blocks)], axis=0)
    counted = jnp.dot(stacked.astype(BF16), before, preferred_element_type=F32)
    base = jnp.zeros((rows, 128), F32)
    ranks = []
    for i in range(blocks):
        block = counted[i * rows : (i + 1) * rows]
        ranks.append(block[:, 0:128] + base)
        base = base + block[:, 128:256]
    return jnp.where(mask > 0.0, jnp.concatenate(ranks, axis=1), -1.0)


def peer_of(me, i, devices):
    if devices & (devices - 1):
        return lax.rem(me + 1 + i, devices)
    return me ^ (devices - 1 - i)


def place_of(device, devices, per_group):
    place = lax.rem(device + per_group // 2, devices)
    return place // per_group, lax.rem(place, per_group)


def section_kernel(
    devices,
    assign_hbm,
    counts_hbm,
    latents_hbm,
    layout_hbm,
    latent_cache_hbm,
    feature_cache_hbm,
    w1_hbm,
    b1_hbm,
    gain_hbm,
    w2_hbm,
    b2_hbm,
    frames_out,
    center,
    first,
    live,
    assign,
    counts,
    latents,
    layout,
    latent_cache,
    feature_cache,
    w1,
    b1,
    gain,
    w2,
    b2,
    halo,
    outgoing,
    incoming,
    past,
    edges,
    row_line,
    row_column,
    row_rank,
    line_mask,
    column_hot,
    feat,
    packed,
    partial,
    pre,
    turn,
    w1_turned,
    mix,
    columns,
    load_sem,
    send_sem,
    recv_sem,
    edge_send,
    edge_recv,
    halo_send,
    halo_recv,
):
    me = lax.axis_index("seq")
    per_group = devices // REQS
    slots = layout.shape[1]
    history, inner, wide = latent_cache.shape
    height = inner * per_group
    span = min(3, per_group)
    starts = per_group - span + 1
    used = -(-span * (slots // devices) // 16) * 16
    lines = FMAX * (inner + 4)
    group, position = place_of(me, devices, per_group)
    above = lax.rem(me + devices - 1, devices)
    below = lax.rem(me + 1, devices)

    barrier = pltpu.get_barrier_semaphore()

    loads = [
        pltpu.make_async_copy(source, target, load_sem.at[i])
        for i, (source, target) in enumerate(
            (
                (assign_hbm, assign),
                (layout_hbm, layout),
                (latents_hbm, latents),
                (latent_cache_hbm, latent_cache),
                (counts_hbm, counts),
                (feature_cache_hbm, feature_cache),
                (w2_hbm, w2),
                (w1_hbm, w1),
                (b1_hbm, b1),
                (gain_hbm, gain),
                (b2_hbm, b2),
            )
        )
    ]
    for load in loads[0:4]:
        load.start()

    def greet(i):
        pl.semaphore_signal(barrier, inc=1, device_id={"seq": peer_of(me, i, devices)})

    trips(devices - 1, greet)

    for load in loads[4:]:
        load.start()


    for load in loads[0:4]:
        load.wait()

    for f in range(history):
        stacked = []
        for r in range(inner):
            row = jnp.broadcast_to(latent_cache[f, r : r + 1, :].astype(F32), (LAT_CH, wide))
            mine = sublane_index(row.shape) == lane_index(row.shape) % LAT_CH
            stacked.append(jnp.where(mine, row, 0.0).astype(BF16))
        pick = sublane_index((wide, 128)) // LAT_CH == lane_index((wide, 128)) % W
        turned = jnp.dot(
            jnp.concatenate(stacked, axis=0), pick.astype(BF16), preferred_element_type=F32
        ).astype(BF16)
        for r in range(0, inner, 2):
            low = turned[r * LAT_CH : (r + 1) * LAT_CH]
            high = turned[(r + 1) * LAT_CH : (r + 2) * LAT_CH]
            left = lane_index(low.shape) < W
            past[f, r // 2] = jnp.where(left, low, high)

    square = (128, 256)
    earlier = (sublane_index(square) < lane_index(square)) | (lane_index(square) >= 128)
    before = earlier.astype(BF16)
    mine = layout[pl.ds(me, 1), :]
    remain = mine // W
    row = lax.rem(remain, height)
    step = remain // height
    windows = REQS * starts
    window = sublane_index((windows, slots))
    request = jnp.zeros((windows, slots), jnp.int32)
    for g in range(REQS):
        request = jnp.where(window // starts == g, assign[g], request)
    low = lax.rem(window, starts) * inner
    member = (step >= request * FMAX) & (step < request * FMAX + FMAX)
    member = member & (row >= low) & (row < low + span * inner)
    rank = ranks_in(jnp.where(member, 1.0, 0.0), before)
    row_rank[0:windows] = rank

    def chosen(i):
        ranked = row_rank[pl.ds(i, 1), :]
        hot = sublane_index((used, slots)).astype(F32) == ranked
        hot = jnp.where(hot, 1.0, 0.0).astype(BF16)
        if used < 128:
            hot = jnp.concatenate([hot, jnp.zeros((128 - used, slots), BF16)], axis=0)
        return hot

    def collect(i):
        hot = jnp.concatenate([chosen(2 * i), chosen(2 * i + 1)], axis=0)
        moved = lax.dot_general(
            latents[...], hot, (((1,), (1,)), ((), ())), preferred_element_type=F32
        ).astype(BF16)
        outgoing[2 * i] = moved[:, 0:128]
        outgoing[2 * i + 1] = moved[:, 128:256]

    trips(windows // 2, collect)

    pl.semaphore_wait(barrier, devices - 1)

    def window_of(device):
        g, k = place_of(device, devices, per_group)
        return g * starts + jnp.clip(k - 1, 0, starts - 1)

    def copy_to(i):
        peer = peer_of(me, i, devices)
        return pltpu.make_async_remote_copy(
            src_ref=outgoing.at[window_of(peer)],
            dst_ref=incoming.at[me],
            send_sem=send_sem.at[peer],
            recv_sem=recv_sem.at[me],
            device_id={"seq": peer},
        )

    def edge_copies(side):
        peer = (above, below)[side]
        copies = []
        for f in range(history):
            copies.append(
                pltpu.make_async_remote_copy(
                    src_ref=past.at[f, 0 if side == 0 else inner // 2 - 1],
                    dst_ref=edges.at[1 - side, f],
                    send_sem=edge_send.at[side, f],
                    recv_sem=edge_recv.at[1 - side, f],
                    device_id={"seq": peer},
                )
            )
            copies.append(
                pltpu.make_async_remote_copy(
                    src_ref=feature_cache.at[f, 0 if side == 0 else inner - 1],
                    dst_ref=halo.at[1 - side, f],
                    send_sem=halo_send.at[side, f],
                    recv_sem=halo_recv.at[1 - side, f],
                    device_id={"seq": peer},
                )
            )
        return copies

    has = (position > 0, position < per_group - 1)
    for side in range(2):

        @pl.when(has[side])
        def _edges():
            for copy in edge_copies(side)[0::2]:
                copy.start()

    trips(devices - 1, lambda i: copy_to(i).start())
    for load in loads[4:6]:
        load.wait()
    for side in range(2):

        @pl.when(has[side])
        def _start():
            for copy in edge_copies(side)[1::2]:
                copy.start()

    incoming[me] = outgoing[window_of(me)]

    number = layout[...]
    remain = number // W
    row = lax.rem(remain, height)
    step = remain // height - assign[group] * FMAX
    first_tile = jnp.clip(position - 1, 0, starts - 1)
    member = (step >= 0) & (step < FMAX)
    member = member & (row >= first_tile * inner) & (row < (first_tile + span) * inner)
    rank = ranks_in(jnp.where(member, 1.0, 0.0), before)
    local = row - (position * inner - 2)
    line = jnp.where((local >= 0) & (local < inner + 4), step * (inner + 4) + local + 1, 0)
    row_rank[0:devices] = rank
    row_line[...] = line.astype(F32)
    row_column[...] = lax.rem(number, W).astype(F32)

    def locate(i):
        ranked = row_rank[pl.ds(i, 1), :]
        hot = sublane_index((128, slots)).astype(F32) == ranked
        hot = jnp.where(hot, 1.0, 0.0).astype(BF16)
        shape = (16, slots)
        what = jnp.where(
            sublane_index(shape) == 0, row_line[pl.ds(i, 1), :], row_column[pl.ds(i, 1), :]
        ).astype(BF16)
        found = lax.dot_general(what, hot, (((1,), (1,)), ((), ())), preferred_element_type=F32)
        level = sublane_index((lines * LAT_CH, 128)) // LAT_CH + 1
        line_mask[i] = jnp.where(level.astype(F32) == found[0:1], 1.0, 0.0).astype(BF16)
        column = jnp.transpose(jnp.broadcast_to(found[1:2], (128, 128)))
        same = column == (lane_index((128, 128)) % W).astype(F32)
        column_hot[pl.ds(pl.multiple_of(i * 128, 128), 128)] = jnp.where(same, 1.0, 0.0).astype(BF16)

    trips(devices, locate)

    mid = feature_cache.shape[3]
    width = b2.shape[0]
    cells = inner * W
    stretch = (inner + 2) * W
    shifted = (feat.at[0], center, feat.at[1])

    def edge_mask(lanes):
        col = lane_index((16, lanes)) % W
        return ((col != 0).astype(BF16), None, (col != W - 1).astype(BF16))

    keep = edge_mask(stretch)

    def spread(f, value, ch):
        for e in range(3):
            moved = value if e == 1 else pltpu.roll(value, (1, 0, stretch - 1)[e], 1) * keep[e]
            shifted[e][f, ch : ch + 16, 0:stretch] = moved

    def spread_inner(f, value, ch):
        for e in range(3):
            moved = value if e == 1 else pltpu.roll(value, (1, 0, cells - 1)[e], 1) * keep[e][:, 0:cells]
            shifted[e][f, ch : ch + 16, stretch : stretch + cells] = moved

    def pack(i):
        at = pl.multiple_of(i * 16, 16)
        for a in range(3):
            taps = [[w2[a, b, e, pl.ds(at, 16), :] for e in range(3)] for b in range(3)]
            add = lambda r, e, q, d: taps[r][e] + taps[q][d]
            for py in range(2):
                edge = 2 * py
                top, low = (1, 2) if py == 0 else (0, 1)
                both = [taps[top][e].astype(F32) + taps[low][e].astype(F32) for e in range(3)]
                for px in range(2):
                    one, near, far = (0, 1, 2) if px == 0 else (2, 0, 1)
                    values = (
                        (add(top, one, low, one), both[near] + both[far]),
                        (taps[edge][one], add(edge, near, edge, far)),
                    )
                    for side in range(2):
                        for which in range(2):
                            ix = which if px == 0 else 1 - which
                            start = ((side * 3 + a) * 2 + ix) * mid
                            packed[2 * py + px, pl.ds(at, 16), start : start + mid] = values[side][which].astype(BF16)

    for load in loads[6:]:
        load.wait()
    lax.fori_loop(0, width // 16, lambda i, c: pack(i) or 0, 0)
    columns[0, 0:mid] = column_of(b1[...].reshape(1, mid), 128)
    columns[1, 0:mid] = column_of(gain[...].reshape(1, mid), 128)
    columns[2, 0:width] = column_of(b2[...].reshape(1, width), 128)
    pair = 2 * W
    spot = sublane_index((2 * pair, 2 * pair))
    goal = spot // pair + 2 * (spot % pair)
    w1_turned[...] = jnp.transpose(w1[...].reshape(27 * LAT_CH, mid).astype(F32)).astype(BF16)
    mix[...] = (lane_index((2 * pair, 2 * pair)) == goal).astype(BF16)
    request = assign[group]
    count = jnp.int32(0)
    for r in range(REQS):
        count = count + jnp.where(request == r, counts[r], 0)
    live[...] = jnp.full(live.shape, count, jnp.int32)

    for f in range(history):
        pre[:, 0:cells] = jnp.transpose(feature_cache[f].reshape(cells, mid).astype(F32))
        for ch in range(0, mid, 16):
            spread_inner(f, pre[ch : ch + 16, 0:cells].astype(BF16), ch)

    def convolve(t, phase, pieces):
        py, px = phase // 2, phase % 2
        total = None
        for side, first_a, last_a in pieces:
            parts = []
            for a in range(first_a, last_a):
                for ix in range(2):
                    begin = stretch if side == 0 else (0 if py == 0 else 2 * W)
                    parts.append(shifted[px + ix][t + a, :, begin : begin + cells])
            begin, end = (side * 3 + first_a) * 2 * mid, (side * 3 + last_a) * 2 * mid
            product = jnp.dot(
                packed[phase, :, begin:end], jnp.concatenate(parts, axis=0), preferred_element_type=F32
            )
            total = product if total is None else total + product
        return total

    for t in range(history):
        for phase in range(4):
            partial[t, phase] = convolve(t, phase, ((0, 0, history - t),))

    for side in range(2):

        @pl.when(jnp.logical_not(has[side]))
        def _clear():
            edges[side] = jnp.zeros(edges.shape[1:], BF16)

        @pl.when(has[side])
        def _arrive():
            for copy in edge_copies(1 - side)[0::2]:
                copy.wait_recv()

    def arrive(i):
        peer = peer_of(me, i, devices)
        pltpu.make_async_remote_copy(
            src_ref=outgoing.at[0],
            dst_ref=incoming.at[peer],
            send_sem=send_sem.at[peer],
            recv_sem=recv_sem.at[peer],
            device_id={"seq": peer},
        ).wait_recv()

    trips(devices - 1, arrive)

    def place(i, total):
        pieces = []
        for half in range(2):
            got = incoming[2 * i + half]
            pieces.append(jnp.concatenate([got] * lines, axis=0) * line_mask[2 * i + half])
        hot = column_hot[pl.ds(pl.multiple_of(i * 256, 256), 256)]
        return total + jnp.dot(jnp.concatenate(pieces, axis=1), hot, preferred_element_type=F32)

    pairs = devices // 2
    placed = lax.fori_loop(
        0,
        pairs,
        place,
        jnp.zeros((lines * LAT_CH, 128), F32),
        unroll=True if pairs <= 16 else 1,
    )
    left = lane_index((LAT_CH, 128)) < W
    block = (inner + 4) * W
    for i in range(lines // 2):
        low = placed[2 * i * LAT_CH : (2 * i + 1) * LAT_CH]
        high = placed[(2 * i + 1) * LAT_CH : (2 * i + 2) * LAT_CH]
        start = history * block + i * 128
        first[:, start : start + 128] = jnp.where(left, low, high).astype(BF16)
    for f in range(history):
        first[:, f * block : f * block + 128] = edges[0, f]
        for r in range(inner // 2):
            start = f * block + 128 + r * 128
            first[:, start : start + 128] = past[f, r]
        first[:, f * block + block - 128 : f * block + block] = edges[1, f]

    value = first[...].astype(F32)
    total = value.shape[1]
    col = lane_index(value.shape) % W
    left = jnp.where(col == 0, 0.0, pltpu.roll(value, 1, 1))
    right = jnp.where(col == W - 1, 0.0, pltpu.roll(value, total - 1, 1))
    shifts = [v.astype(BF16) for v in (left, value, right)]
    later = [pltpu.roll(v, total - W, 1).astype(BF16) for v in (left, value, right)]
    row = lane_index((16, stretch)) // W
    outside = (row == 0) & jnp.logical_not(has[0])
    outside = outside | ((row == inner + 1) & jnp.logical_not(has[1]))
    inside = jnp.where(outside, 0.0, 0.5)
    bias = jnp.concatenate([columns[2, 0:width]] * (cells // 128), axis=1)
    def first_conv(t):
        patch = []
        for a in range(3):
            for b in range(3):
                for e in range(3):
                    source = later[e] if b == 1 else shifts[e]
                    begin = (t + a) * block + (0 if b == 1 else b * W)
                    patch.append(source[:, begin : begin + stretch])
        pre[:, t * stretch : (t + 1) * stretch] = jnp.dot(
            w1_turned[...], jnp.concatenate(patch, axis=0), preferred_element_type=F32
        )

    repeat = lambda x: jnp.concatenate([x] * (stretch // 128), axis=1)
    biased = lambda t, ch: pre[ch : ch + 16, t * stretch : (t + 1) * stretch] + repeat(
        columns[0, ch : ch + 16]
    )

    def norms(t):
        squares = jnp.zeros((16, stretch), F32)
        for ch in range(0, mid, 16):
            x = biased(t, ch)
            squares = squares + x * x
        inverse = lax.rsqrt(jnp.sum(squares, axis=0, keepdims=True) / mid + 1e-06)
        return jnp.broadcast_to(inverse, (16, stretch))

    def activate(t, inverse, chs):
        for ch in chs:
            x = biased(t, ch) * inverse * repeat(columns[1, ch : ch + 16])
            y = x * inside
            y = (y + y * jnp.tanh(0.5 * x)).astype(BF16)
            spread(history + t, y, ch)
            own = pltpu.roll(y, stretch - W, 1)[:, 0:cells]
            spread_inner(history + t, own, ch)

    steps = list(range(0, mid, 16))
    first_conv(0)
    scale_0 = norms(0)
    for t in range(1, FMAX):
        first_conv(t)
        activate(0, scale_0, steps[(t - 1) * len(steps) // (FMAX - 1) : t * len(steps) // (FMAX - 1)])
    alive = live[0:1, :]
    def emit(t, pieces):
        shown = jnp.broadcast_to(alive, (width, pair)) > t
        held = []
        for phase in range(4):
            result = convolve(t, phase, pieces)
            if t < history:
                result = result + partial[t, phase]
            held.append((result + bias).astype(BF16))
            if phase % 2 == 0:
                continue
            for i in range(0, inner, 2):
                both = jnp.concatenate([half[:, i * W : i * W + pair] for half in held], axis=1)
                mixed = jnp.dot(both, mix[...], preferred_element_type=F32)
                for j in range(2):
                    kept = jnp.where(shown, mixed[:, j * pair : (j + 1) * pair], 0.0)
                    frames_out[t, 2 * (i + j) + phase // 2] = kept.astype(BF16)
            held = []

    for t in range(FMAX):
        if t < history:
            following = norms(t + 1)
            for phase in range(4):
                fresh = convolve(t, phase, ((0, history - t, 3), (1, history - t, 3)))
                partial[t, phase] = partial[t, phase] + fresh
                activate(t + 1, following, steps[phase * len(steps) // 4 : (phase + 1) * len(steps) // 4])
        else:
            emit(t, ((0, 0, 3), (1, 0, 3)))
    for side in range(2):

        @pl.when(has[side])
        def _halo():
            for copy in edge_copies(1 - side)[1::2]:
                copy.wait_recv()

    for f in range(history):
        sides = [jnp.where(has[i], halo[i, f], jnp.zeros((), BF16)) for i in range(2)]
        tall = jnp.concatenate([sides[0], feature_cache[f].reshape(cells, mid), sides[1]], axis=0)
        turn[:, 0:stretch] = jnp.transpose(tall.astype(F32))
        for ch in range(0, mid, 16):
            spread(f, turn[ch : ch + 16, 0:stretch].astype(BF16), ch)

    for t in range(history):
        emit(t, ((1, 0, history - t),))

    trips(devices - 1, lambda i: copy_to(i).wait_send())
    for side in range(2):

        @pl.when(has[side])
        def _sent():
            for copy in edge_copies(side):
                copy.wait_send()


def finish_kernel(frames, center, first, live, out, carry, latent_next, carry_buf, latent_buf, sems):
    history, inner, _, mid = carry.shape
    cells = inner * W
    block = (inner + 4) * W
    stores = []

    def store(source, target):
        copy = pltpu.make_async_copy(source, target, sems.at[len(stores)])
        copy.start()
        stores.append(copy)

    for t in range(FMAX):
        store(frames.at[t], out.at[t])

    def picked(values):
        count = jnp.broadcast_to(live[0:1, 0:1], values[0].shape)
        result = values[0]
        for n in range(1, FMAX):
            result = jnp.where(count == n + 1, values[n], result)
        return result

    for i in range(history):
        begin = (inner + 2) * W
        choice = [center[1 + n + i, :, begin : begin + cells].astype(F32) for n in range(FMAX)]
        carry_buf[i] = jnp.transpose(picked(choice)).astype(BF16).reshape(inner, W, mid)
    store(carry_buf, carry)
    parts = []
    for i in range(history):
        start = (1 + i) * block + 2 * W
        choice = [first[:, start + n * block : start + n * block + cells].astype(F32) for n in range(FMAX)]
        own = picked(choice)
        for r in range(inner):
            parts.append(own[:, r * W : (r + 1) * W])
    stacked = jnp.concatenate(parts, axis=0).astype(BF16)
    shape = (W, W * LAT_CH)
    pick = sublane_index(shape) == lane_index(shape) // LAT_CH
    wide = jnp.dot(stacked, pick.astype(BF16), preferred_element_type=F32)
    wide = wide.reshape(history * inner, LAT_CH, W * LAT_CH)
    mine = sublane_index(wide.shape) == lane_index(wide.shape) % LAT_CH
    latent_buf[...] = (
        jnp.sum(jnp.where(mine, wide, 0.0), axis=1).astype(BF16).reshape(history, inner, W * LAT_CH)
    )
    store(latent_buf, latent_next)
    for copy in stores:
        copy.wait()


def section(assign, counts, latents, layout, latent_cache, feature_cache, w1, b1, gain, w2, b2):
    devices, slots = layout.shape
    history, inner, _, mid = feature_cache.shape
    width = b2.shape[0]
    per_group = devices // REQS
    windows = REQS * (per_group - min(3, per_group) + 1)
    lines = FMAX * (inner + 4)
    cells = inner * W
    stretch = (inner + 2) * W
    vmem = pl.BlockSpec(memory_space=pltpu.VMEM)
    hbm = pl.BlockSpec(memory_space=pltpu.HBM)
    inputs = (assign, counts, latents, layout, latent_cache, feature_cache, w1, b1, gain, w2, b2)
    frames, center, first, live = pl.pallas_call(
        functools.partial(section_kernel, devices),
        in_specs=[hbm] * len(inputs),
        out_specs=[vmem] * 4,
        out_shape=[
            jax.ShapeDtypeStruct((FMAX, 2 * inner, width, 2 * W), BF16),
            jax.ShapeDtypeStruct((history + FMAX, mid, stretch + cells), BF16),
            jax.ShapeDtypeStruct((LAT_CH, (history + FMAX) * (inner + 4) * W), BF16),
            jax.ShapeDtypeStruct((8, 128), jnp.int32),
        ],
        scratch_shapes=[(pltpu.SMEM if i < 2 else pltpu.VMEM)(x.shape, x.dtype) for i, x in enumerate(inputs)]
        + [
            pltpu.VMEM((2, history, W, mid), BF16),
            pltpu.VMEM((windows, LAT_CH, 128), BF16),
            pltpu.VMEM((devices, LAT_CH, 128), BF16),
            pltpu.VMEM((history, inner // 2, LAT_CH, 128), BF16),
            pltpu.VMEM((2, history, LAT_CH, 128), BF16),
            pltpu.VMEM((devices, slots), F32),
            pltpu.VMEM((devices, slots), F32),
            pltpu.VMEM((max(devices, windows), slots), F32),
            pltpu.VMEM((devices, lines * LAT_CH, 128), BF16),
            pltpu.VMEM((devices * 128, 128), BF16),
            pltpu.VMEM((2, history + FMAX, mid, stretch + cells), BF16),
            pltpu.VMEM((4, width, 12 * mid), BF16),
            pltpu.VMEM((history, 4, width, cells), F32),
            pltpu.VMEM((mid, FMAX * stretch), F32),
            pltpu.VMEM((mid, stretch), F32),
            pltpu.VMEM((mid, 27 * LAT_CH), BF16),
            pltpu.VMEM((4 * W, 4 * W), BF16),
            pltpu.VMEM((3, mid, 128), F32),
            pltpu.SemaphoreType.DMA((len(inputs),)),
            pltpu.SemaphoreType.DMA((devices,)),
            pltpu.SemaphoreType.DMA((devices,)),
            pltpu.SemaphoreType.DMA((2, history)),
            pltpu.SemaphoreType.DMA((2, history)),
            pltpu.SemaphoreType.DMA((2, history)),
            pltpu.SemaphoreType.DMA((2, history)),
        ],
        compiler_params=pltpu.CompilerParams(
            collective_id=0, has_side_effects=True, vmem_limit_bytes=44 * 1024 * 1024
        ),
    )(*[in_hbm(x) for x in inputs])
    return pl.pallas_call(
        finish_kernel,
        in_specs=[vmem] * 4,
        out_specs=[hbm] * 3,
        out_shape=[
            jax.ShapeDtypeStruct((FMAX, 2 * inner, width, 2 * W), BF16),
            jax.ShapeDtypeStruct((history, inner, W, mid), BF16),
            jax.ShapeDtypeStruct((history, inner, W * LAT_CH), BF16),
        ],
        scratch_shapes=[
            pltpu.VMEM((history, inner, W, mid), BF16),
            pltpu.VMEM((history, inner, W * LAT_CH), BF16),
            pltpu.SemaphoreType.DMA((FMAX + 2,)),
        ],
        compiler_params=pltpu.CompilerParams(vmem_limit_bytes=16 * 1024 * 1024),
    )(frames, center, first, live)


def body(
    latents,
    layout,
    assign,
    counts,
    latent_cache,
    feature_cache,
    first_weight,
    first_bias,
    norm_gain,
    second_weight,
    second_bias,
):
    decoded_frames, feature_next, latent_next = section(
        assign,
        counts,
        latents,
        layout,
        latent_cache,
        feature_cache,
        first_weight,
        first_bias,
        norm_gain,
        jnp.swapaxes(second_weight, 3, 4),
        second_bias,
    )
    return (jnp.swapaxes(decoded_frames, 2, 3), latent_next, feature_next)


def solution(mesh):
    return jax.shard_map(
        body,
        mesh=mesh,
        in_specs=(
            P(None, ("rep", "seq")),
            P("rep", None),
            P("rep"),
            P("rep"),
            P(None, ("rep", "seq"), None),
            P(None, ("rep", "seq"), None, None),
            P(),
            P(),
            P(),
            P(),
            P(),
        ),
        out_specs=(
            P(None, ("rep", "seq"), None, None),
            P(None, ("rep", "seq"), None),
            P(None, ("rep", "seq"), None, None),
        ),
        check_vma=False,
    )
```
